1024 devices in a mesh: dom: 256 (over z, y, core), grp: 4 (over x).
Axes of the slice: x: 4, y: 8, z: 16, core: 2. Of those that a mesh axis runs over, the one named last changes fastest.
Arguments:
- positions: float32 [3, 1048576], P(None, ('dom', 'grp')), may hold values from 0 to 65, as said below
- velocity: float32 [3, 1048576], P(None, ('dom', 'grp')), may hold values from -6 to 6
- smoothing: float32 [1048576], P(('dom', 'grp')), may hold values from 0.24 to 0.4
- mass: float32 [1048576], P(('dom', 'grp')), may hold values from 0.002 to 0.02
- energy: float32 [1048576], P(('dom', 'grp')), may hold values from 0.5 to 4
- targets: int32 [8192, 1], P(('dom', 'grp')), may hold values from 0 to 3; in each aligned block of 8 rows (0 to 7, 8 to 15, ...) at most 4 rows name the same one
- neighbours: int32 [8192, 4], P(('dom', 'grp')), may hold values from 0 to 143
- counts: int32 [8192], P(('dom', 'grp')), may hold values from 1 to 128
Outputs:
- density: float32 [2097152], P(('dom', 'grp'))
- accel: float32 [3, 2097152], P(None, ('dom', 'grp'))
- timestep: float32 [1], replicated
The draws below stay inside these ranges and needn't reach their ends.
Inputs may be any that keep to these rules, and one draw needn't show every extreme that they name: `targets`: each device sends at most 4 blocks to one index of grp, and exactly 4 in some draws' devices. `positions`: the particles of a block of a device with index a along dom have first component within a / 4 to a / 4 + 1, the others within 0 to 1.
All inputs are finite; a program needn't handle non-finite values.
Results may differ from the reference program's by a relative error of at most 0.0003.
Values sent between devices are 32-bit elements; how exact they have to be, the bound alone decides.
A program may use at most 32 MiB of HBM per device.

```python
import math
import jax
import jax.numpy as jnp
import numpy as np
from jax import lax

BLOCK = 128
NBLK = 8
NBR = 4
CAP = 4
BLOCKS = 8192
PART = 1048576
N_DOM = 256
N_GRP = 4


def draw_positions(key, part):
    first_key = jax.random.fold_in(key, 11)
    within = jax.random.uniform(first_key, (3, PART), jnp.float32)
    index = jnp.arange(PART, dtype=jnp.int32)
    domain = 0.25 * (index // (BLOCK * NBLK * N_GRP)).astype(jnp.float32)
    offset = jnp.stack([domain, jnp.zeros_like(domain), jnp.zeros_like(domain)], axis=0)
    return within + offset


def touch_ends(values, stream_key, low, largest):
    shape = values.shape
    place = [jax.random.randint(jax.random.fold_in(stream_key, axis), (), 0, shape[axis]) for axis in range(len(shape))]
    values = values.at[tuple(place)].set(low)
    longest = shape.index(max(shape))
    place[longest] = (place[longest] + 1) % shape[longest]
    return values.at[tuple(place)].set(largest)


def shard_levels(own_key, dims, shards, least, high):
    def one(axis_at, shards_of):
        draws = jax.random.uniform(jax.random.fold_in(jax.random.fold_in(own_key, 6), axis_at), (shards_of,), jnp.float32, least / len(shards), high / len(shards))
        return jnp.repeat(jnp.exp(draws), dims[axis_at] // shards_of).reshape((-1,) + (1,) * (len(dims) - axis_at - 1))

    gain = one(*shards[0])
    for cut in shards[1:]:
        gain = gain * one(*cut)
    return gain


def shared_out(key, own, number, rows, count, top, bound, lean):
    sequence = jax.random.permutation(key, count)
    heavy_load, ordinary = load_shares(count, rows * top, bound, lean, True), load_shares(count, rows * top, bound, lean, False)
    places = jnp.arange(count)

    def named(lengths, rotation):
        used = int((lengths > 0).sum())
        fixed = max(1, used // 4)
        passed = fixed + (places - fixed + rotation * (used - fixed)) % max(1, count - fixed)
        return jnp.zeros((count,), jnp.int32).at[sequence[jnp.where(places < fixed, places, passed)]].set(jnp.asarray(lengths, jnp.int32))

    lengths = jnp.where(number % 4 == 0, named(heavy_load, number // 4), named(ordinary, number - number // 4 - 1))
    mixed = jax.random.permutation(jax.random.fold_in(own, 3), count)
    donor, receiver = mixed[0:count // 2 * 2:2], mixed[1:count // 2 * 2:2]
    room = jnp.minimum(lengths[donor] - 1, bound - lengths[receiver]) // 2
    room = jnp.where((donor == sequence[0]) | (receiver == sequence[0]) | (lengths[receiver] == 0), 0, jnp.maximum(room, 0))
    passed = jax.random.randint(jax.random.fold_in(own, 4), (count // 2,), 0, 1 << 20) % (room + 1)
    lengths = lengths.at[donor].add(-passed).at[receiver].add(passed)
    items = jnp.searchsorted(jnp.cumsum(lengths), jnp.arange(rows * top), side="right").astype(jnp.int32)
    listing = items.reshape(top, rows).T
    listing = listing[jax.random.permutation(jax.random.fold_in(own, 1), rows)]
    rotation = jax.random.randint(jax.random.fold_in(own, 2), (rows, 1), 0, top)
    return jnp.take_along_axis(listing, (jnp.arange(top)[None, :] + rotation) % top, axis=1)


def load_shares(count, total, reach, lean, full):
    weights = [(1 << 20) // math.isqrt(grade ** lean) + 1 for grade in range(1, count + 1)]
    largest = reach if full else min(reach, max(-(-total // count), total * weights[0] // sum(weights)))
    least = 1 if total - largest >= count - 1 else 0
    given, rest = [largest] + [least] * (count - 1), total - largest - least * (count - 1)
    while rest > 0:
        free = [i for i in range(1, count) if given[i] < largest] or [i for i in range(1, count) if given[i] < reach]
        whole, budget = sum([weights[i] for i in free]), rest
        for i in free:
            addition = min(reach - given[i], max(1, budget * weights[i] // whole), rest)
            given[i] = given[i] + addition
            rest = rest - addition
    return np.array(given)


def gaussian(rng, dims, deviation, bound, split=(), held_as=jnp.bfloat16):
    gain = shard_levels(rng, dims, split, -0.22, 0.18) if split else 1.0
    drawn = jax.random.normal(rng, dims, jnp.float32) * deviation * gain
    return jnp.minimum(jnp.maximum(drawn, -bound), bound).astype(held_as)


def setup_inputs(seed: int = 0) -> dict:
    key_of = jax.random.split(jax.random.key(seed), 9)
    positions = draw_positions(jax.random.fold_in(key_of[8], 71), 0)
    velocity = gaussian(key_of[1], (3, PART), 1.0, 6.0, ((1, 1024),), jnp.float32)
    smoothing = jnp.clip(jnp.exp(math.log(0.4) - 0.51082566 * jax.random.uniform(key_of[2], (PART,), jnp.float32) ** shard_levels(key_of[2], (PART,), ((0, 1024),), -0.2, 0.2)), 0.24, 0.4)
    mass = jnp.clip(jnp.exp(math.log(0.02) - 2.30258502 * jax.random.uniform(key_of[3], (PART,), jnp.float32) ** shard_levels(key_of[3], (PART,), ((0, 1024),), -0.2, 0.2)), 0.002, 0.02)
    energy = jnp.clip(jnp.exp(math.log(4.0) - 2.0794415 * jax.random.uniform(key_of[4], (PART,), jnp.float32) ** shard_levels(key_of[4], (PART,), ((0, 1024),), -0.2, 0.2)), 0.5, 4.0)
    targets_keys = jax.random.split(jax.random.fold_in(key_of[5], 1), BLOCKS // NBLK)
    targets_turns = jax.random.permutation(jax.random.fold_in(key_of[5], 3), BLOCKS // NBLK)
    targets = jax.vmap(lambda own, number: shared_out(jax.random.fold_in(key_of[5], 2), own, number, NBLK, N_GRP, 1, CAP, 2))(targets_keys, targets_turns).reshape((BLOCKS, 1))
    neighbours = touch_ends(jax.random.randint(key_of[6], (BLOCKS, NBR), 0, 9 * N_GRP * CAP), jax.random.fold_in(key_of[6], 1), 0, (9 * N_GRP * CAP) - 1).astype(jnp.int32)
    counts = touch_ends(jax.random.randint(key_of[7], (BLOCKS,), 1, BLOCK + 1), jax.random.fold_in(key_of[7], 1), 1, BLOCK).astype(jnp.int32)
    return dict(positions=positions, velocity=velocity, smoothing=smoothing, mass=mass, energy=energy, targets=targets, neighbours=neighbours, counts=counts)


DRIFT = 0.05
GAMMA = 5.0 / 3.0
CFL = 0.3
KNORM = 315.0 / (64.0 * math.pi)

def partner_sums(own_x, own_h, part_x, part_m, part_f, own_f):
    dsq = jnp.zeros(part_m.shape[:2] + (own_x.shape[2], part_m.shape[2]), jnp.float32)
    diffs = []
    for comp in range(3):
        delta = own_x[:, None, comp, :, None] - part_x[:, :, comp, None, :]
        diffs.append(delta)
        dsq = dsq + delta * delta
    inv_h = 1.0 / own_h
    base = jnp.maximum(1.0 - dsq * (inv_h * inv_h)[:, None, :, None], 0.0)
    rho = KNORM * inv_h ** 3 * lax.optimization_barrier(jnp.sum(part_m[:, :, None, :] * base ** 3, axis=(1, 3)))
    if part_f is None:
        return rho
    coef = part_m[:, :, None, :] * (own_f[:, None, :, None] + part_f[:, :, None, :]) * base * base
    acc = jnp.stack([lax.optimization_barrier(jnp.sum(coef * diffs[c], axis=(1, 3))) for c in range(3)], axis=1)
    return 6.0 * KNORM * (inv_h ** 5)[:, None, :] * acc

def reference(positions, velocity, smoothing, mass, energy, targets, neighbours, counts):
    devices = N_DOM * N_GRP
    slots = N_GRP * CAP
    drifted = positions + DRIFT * velocity
    fields = jnp.concatenate([drifted, smoothing[None], mass[None], energy[None]], axis=0)
    fields = fields.reshape(6, devices * NBLK, BLOCK).transpose(1, 0, 2)
    target = targets[:, 0].reshape(devices, NBLK)
    onehot = (target[:, :, None] == jnp.arange(N_GRP, dtype=jnp.int32)[None, None, :]).astype(jnp.int32)
    before = jnp.cumsum(onehot, axis=1) - onehot
    rank = lax.optimization_barrier(jnp.sum(before * onehot, axis=2))
    source = jnp.arange(devices, dtype=jnp.int32)[:, None]
    new_dev = source // N_GRP * N_GRP + target
    new_slot = source % N_GRP * CAP + rank
    where_to = (new_dev * slots + new_slot).reshape(-1)
    slot_fields = jnp.zeros((devices * slots, 6, BLOCK), jnp.float32).at[where_to].set(fields)
    slot_nbr = jnp.zeros((devices * slots, NBR), jnp.int32).at[where_to].set(neighbours)
    slot_cnt = jnp.zeros((devices * slots,), jnp.int32).at[where_to].set(counts)
    live = slot_cnt > 0
    hval = jnp.where(live[:, None], slot_fields[:, 3], 1.0)
    grid = slot_fields[:, jnp.array([0, 1, 2, 4])].reshape(N_DOM, N_GRP, slots, 4, BLOCK)
    grid = jnp.pad(grid, ((1, 1), (1, 1), (0, 0), (0, 0), (0, 0)))
    own_index = 4 * slots + jnp.arange(slots, dtype=jnp.int32)

    def pool_of(dev, table, tail):
        start = (dev // N_GRP, dev % N_GRP) + (0,) * (table.ndim - 2)
        start = tuple((jnp.asarray(v).astype(jnp.int32) for v in start))
        return lax.dynamic_slice(table, start, (3, 3, slots) + tail).reshape((9 * slots,) + tail)

    def partners(dev):
        nbr = lax.dynamic_slice_in_dim(slot_nbr, (dev * slots).astype(jnp.int32), slots, 0)
        return jnp.concatenate([own_index[:, None], nbr], axis=1)

    def first_pass(dev):
        pool = pool_of(dev, grid, (4, BLOCK))
        idx = partners(dev)
        own = lax.dynamic_slice_in_dim(slot_fields, (dev * slots).astype(jnp.int32), slots, 0)
        own_h = lax.dynamic_slice_in_dim(hval, (dev * slots).astype(jnp.int32), slots, 0)
        chosen = pool[idx]
        return partner_sums(own[:, 0:3], own_h, chosen[:, :, 0:3], chosen[:, :, 3], None, None)
    rho = lax.map(first_pass, jnp.arange(devices, dtype=jnp.int32)).reshape(devices * slots, BLOCK)
    rho_safe = jnp.where(live[:, None], rho, 1.0)
    factor = jnp.where(live[:, None], (GAMMA - 1.0) * slot_fields[:, 5] / rho_safe, 0.0)
    fgrid = jnp.pad(factor.reshape(N_DOM, N_GRP, slots, BLOCK), ((1, 1), (1, 1), (0, 0), (0, 0)))

    def second_pass(dev):
        pool = pool_of(dev, grid, (4, BLOCK))
        fpool = pool_of(dev, fgrid, (BLOCK,))
        idx = partners(dev)
        own = lax.dynamic_slice_in_dim(slot_fields, (dev * slots).astype(jnp.int32), slots, 0)
        own_h = lax.dynamic_slice_in_dim(hval, (dev * slots).astype(jnp.int32), slots, 0)
        own_f = lax.dynamic_slice_in_dim(factor, (dev * slots).astype(jnp.int32), slots, 0)
        chosen = pool[idx]
        return partner_sums(own[:, 0:3], own_h, chosen[:, :, 0:3], chosen[:, :, 3], fpool[idx], own_f)
    acc = lax.map(second_pass, jnp.arange(devices, dtype=jnp.int32)).reshape(devices * slots, 3, BLOCK)
    active = jnp.arange(BLOCK, dtype=jnp.int32)[None, :] < slot_cnt[:, None]
    acc = jnp.where(active[:, None, :], acc, 0.0)
    density = jnp.where(live[:, None], rho, 0.0).reshape(-1)
    accel = acc.transpose(1, 0, 2).reshape(3, -1)
    sound = jnp.sqrt(GAMMA * (GAMMA - 1.0) * jnp.where(active, slot_fields[:, 5], 1.0))
    steps_each = jnp.where(active, CFL * hval / sound, 1e+30)
    timestep = jnp.min(steps_each).reshape(1)
    return (density, accel, timestep)
```

```python
import functools
import math

import jax
import jax.numpy as jnp
from jax import lax
from jax.experimental import pallas as pl
from jax.experimental.pallas import tpu as pltpu
from jax.sharding import PartitionSpec as P

MESH = pl.DeviceIdType.MESH
CAP = 4
DRIFT = 0.05
GAMMA = 5.0 / 3.0
CFL = 0.3
KNORM = 315.0 / (64.0 * math.pi)

NB = 8
NG = 4
NZ, NY = 16, 8
W = 128
EMPTY = 12 * NB
CH = 32


def at(dom, grp):
    return {"dom": dom, "grp": grp}


def remote(src, dst, send, recv, to):
    return pltpu.make_async_remote_copy(
        src_ref=src, dst_ref=dst, send_sem=send, recv_sem=recv, device_id=to, device_id_type=MESH
    )


def landed(ref, sem):
    pltpu.make_async_copy(ref, ref, sem).wait()


def kernel(
    tgt, nbr, cnt, pos, vel, smooth, mass, energy, dens_out, acc_out, ts_out,
    pool, mfpool, table, rows, cols, coll, res, outsend, outbuf,
    mine, zbuf, ybuf, xbuf, ysrc, xsrc, last, final,
    dsend, drecv, tsend, trecv, fsend, frecv, osend, orecv, msend, mrecv,
):
    a = lax.axis_index("dom")
    g = lax.axis_index("grp")
    n_dom = lax.axis_size("dom")
    z, y, c = a // 16, (a // 2) % 8, a % 2
    root = z < 2
    low, high = a > 0, a < n_dom - 1

    def dom_of(zz, yy, cc):
        return (zz * NY + yy) * 2 + cc

    others = [lax.rem(g + d, NG) for d in (2, 1, 3)]
    y_peers = [at(dom_of(z, lax.rem(y + d, NY), c), g) for d in (4, 3, 5, 2, 6, 1, 7)]
    x_peers = [
        at(dom_of(z, y, lax.rem(c + dc, 2)), lax.rem(g + dx, NG))
        for dx in (2, 1, 3, 0) for dc in (0, 1) if dx or dc
    ]

    barrier = pltpu.get_barrier_semaphore()

    def greet(to):
        pl.semaphore_signal(barrier, inc=1, device_id=to, device_id_type=MESH)

    for o in others:
        greet(at(a, o))

    @pl.when(low)
    def _():
        greet(at(a - 1, g))

    @pl.when(high)
    def _():
        greet(at(a + 1, g))

    @pl.when(root)
    def _():
        def child(k, _):
            greet(at(dom_of(k, y, c), g))
            return 0

        lax.fori_loop(2, NZ, child, 0)
        greet(at(dom_of(1 - z, y, c), g))
        for p in y_peers + x_peers:
            greet(p)

    lane = lax.broadcasted_iota(jnp.int32, (NB, W), 1)
    sub = lax.broadcasted_iota(jnp.int32, (NB, W), 0)
    count = jnp.zeros((NB, W), jnp.int32)
    for b in range(NB):
        count = jnp.where(sub == b, cnt[b], count)
    active = lane < count
    h = smooth[...]
    u = energy[...]
    m = mass[...]
    steps = jnp.where(active, CFL * h / jnp.sqrt(GAMMA * (GAMMA - 1.0) * u), 1e30)
    mine[...] = jnp.min(steps, axis=0, keepdims=True)

    own = (NG + g) * 4 * NB
    for comp in range(3):
        for b in range(NB):
            piece = pl.ds(b * W, W)
            rows[comp * NB + b : comp * NB + b + 1, :] = (
                pos[comp : comp + 1, piece] + DRIFT * vel[comp : comp + 1, piece]
            )
        pool[pl.ds(pl.multiple_of(own + comp * NB, NB), NB), :] = rows[comp * NB : comp * NB + NB, :]
    pool[pl.ds(pl.multiple_of(own + 3 * NB, NB), NB), :] = m
    pool[pl.ds(EMPTY * 4, 4 * NB), :] = jnp.zeros((4 * NB, W), jnp.float32)
    mfpool[pl.ds(EMPTY, NB), :] = jnp.zeros((NB, W), jnp.float32)
    res[pl.ds(4 * NB, NB), :] = jnp.zeros((NB, W), jnp.float32)

    targets = [tgt[b] for b in range(NB)]
    ranks = []
    for b in range(NB):
        r = jnp.int32(0)
        for e in range(b):
            r = r + jnp.where(targets[e] == targets[b], 1, 0)
        ranks.append(r)
    places = [targets[b] * CAP + ranks[b] for b in range(NB)]
    for s in range(NG * CAP):
        found = jnp.int32(NB)
        for b in range(NB):
            found = jnp.where(places[b] == s, b, found)
        table[NG + g, s] = found

    @pl.when(jnp.logical_not(low))
    def _():
        for d in range(NG):
            for s in range(NG * CAP):
                table[d, s] = jnp.int32(NB)

    @pl.when(jnp.logical_not(high))
    def _():
        for d in range(NG):
            for s in range(NG * CAP):
                table[2 * NG + d, s] = jnp.int32(NB)

    wait_for = 3 + jnp.where(low, 1, 0) + jnp.where(high, 1, 0) + jnp.where(root, 15, 2)
    pl.semaphore_wait(barrier, wait_for)

    for zr in range(2):
        @pl.when(z != zr)
        def _():
            remote(mine, zbuf.at[pl.ds(z, 1)], msend.at[zr], mrecv.at[0], at(dom_of(zr, y, c), g)).start()

    def group_copies(ref, per, send, recv):
        part = ref.at[pl.ds(pl.multiple_of((NG + g) * per, per), per)]
        return [remote(part, part, send.at[k], recv.at[0], at(a, o)) for k, o in enumerate(others)]

    def side_copy(ref, per, send, recv, up):
        src = ref.at[pl.ds(NG * per, NG * per)]
        dst = ref.at[pl.ds(0 if up else 2 * NG * per, NG * per)]
        return remote(src, dst, send.at[3 if up else 4], recv.at[1 if up else 2], at(a + (1 if up else -1), g))

    def exchange(parts, between=None):
        for part in parts:
            for copy in group_copies(*part):
                copy.start()
        if between is not None:
            between()
        for ref, per, send, recv in parts:
            landed(ref.at[pl.ds(0, 3 * per)], recv.at[0])

        @pl.when(high)
        def _():
            for part in parts:
                side_copy(*part, True).start()

        @pl.when(low)
        def _():
            for part in parts:
                side_copy(*part, False).start()

    def arrived(parts):
        @pl.when(low)
        def _():
            for ref, per, send, recv in parts:
                landed(ref.at[pl.ds(0, NG * per)], recv.at[1])

        @pl.when(high)
        def _():
            for ref, per, send, recv in parts:
                landed(ref.at[pl.ds(0, NG * per)], recv.at[2])

    def sent(parts):
        for part in parts:
            for copy in group_copies(*part):
                copy.wait_send()

        @pl.when(high)
        def _():
            for part in parts:
                side_copy(*part, True).wait_send()

        @pl.when(low)
        def _():
            for part in parts:
                side_copy(*part, False).wait_send()

    first = ((pool, 4 * NB, dsend, drecv), (table, 1, tsend, trecv))
    second = ((mfpool, NB, fsend, frecv),)

    def columns():
        rows[3 * NB : 4 * NB, :] = h * h

        def one(b, _):
            for comp in range(4):
                row = rows[pl.ds(comp * NB + b, 1), :]
                cols[comp, pl.ds(pl.multiple_of(b * W, W), W), :] = jnp.transpose(jnp.broadcast_to(row, (W, W)))
            return 0

        lax.fori_loop(0, NB, one, 0)

    exchange(first, columns)
    arrived(first)

    def partner(b, k):
        if k == 0:
            return NG + g, b
        n = nbr[b * 4 + k - 1]
        cell, s = n // 16, n % 16
        i, j = cell // 3, cell % 3
        t = tgt[b] + j - 1
        d = i * NG + s // CAP
        e = table[d, jnp.clip(t, 0, NG - 1) * CAP + s % CAP]
        there = (t >= 0) & (t < NG) & (a + i >= 1) & (a + i <= n_dom) & (e < NB)
        return jnp.where(there, d, 3 * NG), jnp.where(there, e, 0)

    lane_of = lax.broadcasted_iota(jnp.int32, (CH, W), 1)

    def pairs(second_pass):
        def block(b, _):
            who = [partner(b, k) for k in range(5)]

            def chunk(q, _):
                mine_at = pl.ds(pl.multiple_of(b * W + q * CH, CH), CH)
                cx, cy, cz, ch2 = (cols[comp, mine_at, :] for comp in range(4))
                sums = [jnp.zeros((CH, W), jnp.float32) for _ in range(3 if second_pass else 4)]
                for d, e in who:
                    base = d * (4 * NB) + e
                    dx = cx - pool[pl.ds(base, 1), :]
                    dy = cy - pool[pl.ds(base + NB, 1), :]
                    dz = cz - pool[pl.ds(base + 2 * NB, 1), :]
                    w = jnp.maximum(ch2 - (dx * dx + dy * dy + dz * dz), 0.0)
                    if second_pass:
                        weight = mfpool[pl.ds(d * NB + e, 1), :]
                    else:
                        weight = pool[pl.ds(base + 3 * NB, 1), :]
                    mw = weight * (w * w)
                    parts = [mw * dx, mw * dy, mw * dz]
                    if not second_pass:
                        parts = parts + [mw * w]
                    sums = [s + p for s, p in zip(sums, parts)]
                here = pl.ds(pl.multiple_of(q * CH, CH), CH)
                kept = coll[here, :]
                for k, s in enumerate(sums):
                    kept = jnp.where(lane_of == k * NB + b, jnp.sum(s, axis=1, keepdims=True), kept)
                coll[here, :] = kept
                return 0

            lax.fori_loop(0, W // CH, chunk, 0)
            return 0

        coll[...] = jnp.zeros((W, W), jnp.float32)
        lax.fori_loop(0, NB, block, 0)
        return jnp.transpose(coll[...])

    inv_h = 1.0 / h
    ih3 = inv_h * inv_h * inv_h
    ih9 = KNORM * (ih3 * ih3 * ih3)

    found = pairs(False)
    rho = ih9 * found[3 * NB : 4 * NB, :]
    factor = (GAMMA - 1.0) * u / rho
    mfpool[pl.ds(pl.multiple_of((NG + g) * NB, NB), NB), :] = m * factor
    res[0:NB, :] = rho
    for comp in range(3):
        res[(1 + comp) * NB : (2 + comp) * NB, :] = factor * found[comp * NB : (comp + 1) * NB, :]

    exchange(second)
    arrived(second)

    found = pairs(True)
    for comp in range(3):
        here = slice((1 + comp) * NB, (2 + comp) * NB)
        total = 6.0 * ih9 * (res[here, :] + found[comp * NB : (comp + 1) * NB, :])
        res[here, :] = jnp.where(active, total, 0.0)

    for t in range(NG):
        for r in range(CAP):
            e = table[NG + g, t * CAP + r]
            for comp in range(4):
                source = jnp.where(e < NB, comp * NB + e, 4 * NB)
                outsend[t, comp * CAP + r : comp * CAP + r + 1, :] = res[pl.ds(source, 1), :]
    results = [remote(outsend.at[o], outbuf.at[g], osend.at[k], orecv, at(a, o)) for k, o in enumerate(others)]
    for copy in results:
        copy.start()
    outbuf[g] = outsend[g]
    landed(outbuf.at[pl.ds(0, 3)], orecv)
    for s in range(NG):
        dens_out[s * CAP : (s + 1) * CAP, :] = outbuf[s, 0:CAP, :]
        for comp in range(3):
            for r in range(CAP):
                row = (1 + comp) * CAP + r
                slot = s * CAP + r
                acc_out[comp : comp + 1, slot * W : (slot + 1) * W] = outbuf[s, row : row + 1, :]

    def reduce_and_send(buf, index, value, src, peers, send, recv, slot):
        buf[pl.ds(index, 1), :] = value
        src[...] = value
        for k, p in enumerate(peers):
            remote(src, buf.at[pl.ds(index, 1)], send.at[k], recv, p).start()
        landed(buf.at[pl.ds(0, slot - 1)], recv)
        return jnp.min(buf[...], axis=0, keepdims=True)

    @pl.when(root)
    def _():
        zbuf[pl.ds(z, 1), :] = mine[...]
        landed(zbuf.at[pl.ds(0, NZ - 1)], mrecv.at[0])
        least = jnp.min(zbuf[...], axis=0, keepdims=True)
        least = reduce_and_send(ybuf, y, least, ysrc, y_peers, msend.at[pl.ds(2, 7)], mrecv.at[1], NY)
        least = reduce_and_send(xbuf, c * NG + g, least, xsrc, x_peers, msend.at[pl.ds(9, 7)], mrecv.at[2], 2 * NG)
        last[...] = least

        def child(k, _):
            to = jnp.where(z == 0, NZ - 1 - k, 2 + k)
            remote(last, final, msend.at[16 + k], mrecv.at[3], at(dom_of(to, y, c), g)).start()
            return 0

        lax.fori_loop(0, 7, child, 0)
        final[...] = least
        for k in range(21):
            landed(last, msend.at[2 + k])

    @pl.when(jnp.logical_not(root))
    def _():
        landed(final, mrecv.at[3])

    ts_out[...] = jnp.broadcast_to(jnp.min(final[...], axis=1, keepdims=True), (1, W))

    sent(first)
    sent(second)
    for copy in results:
        copy.wait_send()
    for zr in range(2):
        @pl.when(z != zr)
        def _():
            landed(mine, msend.at[zr])


def body(positions, velocity, smoothing, mass, energy, targets, neighbours, counts):
    f32 = jnp.float32
    slots = NG * CAP
    vmem, smem = pl.BlockSpec(memory_space=pltpu.VMEM), pl.BlockSpec(memory_space=pltpu.SMEM)
    sem = pltpu.SemaphoreType.DMA
    dens, acc, ts = pl.pallas_call(
        kernel,
        out_shape=(
            jax.ShapeDtypeStruct((slots, W), f32),
            jax.ShapeDtypeStruct((3, slots * W), f32),
            jax.ShapeDtypeStruct((1, W), f32),
        ),
        in_specs=[smem] * 3 + [vmem] * 5,
        out_specs=(vmem, vmem, vmem),
        scratch_shapes=[
            pltpu.VMEM(((EMPTY + NB) * 4, W), f32),
            pltpu.VMEM((EMPTY + NB, W), f32),
            pltpu.SMEM((3 * NG, 16), jnp.int32),
            pltpu.VMEM((4 * NB, W), f32),
            pltpu.VMEM((4, NB * W, W), f32),
            pltpu.VMEM((W, W), f32),
            pltpu.VMEM((5 * NB, W), f32),
            pltpu.VMEM((NG, 4 * CAP, W), f32),
            pltpu.VMEM((NG, 4 * CAP, W), f32),
            pltpu.VMEM((1, W), f32),
            pltpu.VMEM((NZ, W), f32),
            pltpu.VMEM((NY, W), f32),
            pltpu.VMEM((2 * NG, W), f32),
            pltpu.VMEM((1, W), f32),
            pltpu.VMEM((1, W), f32),
            pltpu.VMEM((1, W), f32),
            pltpu.VMEM((1, W), f32),
            sem((5,)), sem((3,)), sem((5,)), sem((3,)), sem((5,)), sem((3,)),
            sem((3,)), sem, sem((24,)), sem((4,)),
        ],
        compiler_params=pltpu.CompilerParams(collective_id=0, has_side_effects=True),
    )(
        targets.reshape(-1), neighbours.reshape(-1), counts, positions, velocity,
        smoothing.reshape(NB, W), mass.reshape(NB, W), energy.reshape(NB, W),
    )
    return dens.reshape(-1), acc, ts[0, :1]


def solution(mesh):
    both = ("dom", "grp")
    return jax.shard_map(
        body,
        mesh=mesh,
        in_specs=(P(None, both), P(None, both), P(both), P(both), P(both), P(both, None), P(both, None), P(both)),
        out_specs=(P(both), P(None, both), P()),
        check_vma=False,
    )
```

```python
import functools
import math

import jax
import jax.numpy as jnp
from jax import lax
from jax.experimental import pallas as pl
from jax.experimental.pallas import tpu as pltpu
from jax.sharding import PartitionSpec as P

MESH = pl.DeviceIdType.MESH
CAP = 4
DRIFT = 0.05
GAMMA = 5.0 / 3.0
CFL = 0.3
KNORM = 315.0 / (64.0 * math.pi)

NB = 8
NG = 4
NZ, NY = 16, 8
W = 128
EMPTY = 12 * NB
CH = 32


def at(dom, grp):
    return {"dom": dom, "grp": grp}


def remote(src, dst, send, recv, to):
    return pltpu.make_async_remote_copy(
        src_ref=src, dst_ref=dst, send_sem=send, recv_sem=recv, device_id=to, device_id_type=MESH
    )


def landed(ref, sem):
    pltpu.make_async_copy(ref, ref, sem).wait()


def kernel(
    tgt_in, nbr_in, cnt_in, pos_in, vel_in, smooth_in, mass_in, energy_in, slots_out, least_out,
    tgt, nbr, cnt, pos, vel, smooth, mass, energy, base_of,
    pool, mfpool, table, rows, cols, stash, coll, res, outsend, outbuf,
    mine, zbuf, xbuf, last, final,
    load, dsend, drecv, tsend, trecv, fsend, frecv, osend, orecv, msend, mrecv,
):
    a = lax.axis_index("dom")
    g = lax.axis_index("grp")
    n_dom = lax.axis_size("dom")
    z, y, c = a // 16, (a // 2) % 8, a % 2
    root = z < 2
    low, high = a > 0, a < n_dom - 1

    def dom_of(zz, yy, cc):
        return (zz * NY + yy) * 2 + cc

    others = [lax.rem(g + d, NG) for d in (2, 1, 3)]
    plane = [
        at(dom_of(z, lax.rem(y + dy, NY), lax.rem(c + dc, 2)), lax.rem(g + dx, NG))
        for dy in (4, 3, 5, 2, 6, 1, 7, 0) for dx in (2, 1, 3, 0) for dc in (0, 1) if dy or dx or dc
    ]

    loads = [
        pltpu.make_async_copy(src, dst, load.at[k])
        for k, (src, dst) in enumerate((
            (cnt_in, cnt), (smooth_in, smooth), (energy_in, energy), (tgt_in, tgt),
            (pos_in, pos), (vel_in, vel), (mass_in, mass), (nbr_in, nbr),
        ))
    ]
    for copy in loads:
        copy.start()

    barrier = pltpu.get_barrier_semaphore()

    def greet(to):
        pl.semaphore_signal(barrier, inc=1, device_id=to, device_id_type=MESH)

    for o in others:
        greet(at(a, o))

    @pl.when(low)
    def _():
        greet(at(a - 1, g))

    @pl.when(high)
    def _():
        greet(at(a + 1, g))

    @pl.when(root)
    def _():
        def child(k, _):
            greet(at(dom_of(k, y, c), g))
            return 0

        lax.fori_loop(2, NZ, child, 0)
        greet(at(dom_of(1 - z, y, c), g))
        for p in plane:
            greet(p)

    lane = lax.broadcasted_iota(jnp.int32, (NB, W), 1)
    sub = lax.broadcasted_iota(jnp.int32, (NB, W), 0)
    for copy in loads[:3]:
        copy.wait()
    count = jnp.zeros((NB, W), jnp.int32)
    for b in range(NB):
        count = jnp.where(sub == b, cnt[b], count)
    active = lane < count
    h = smooth[...]
    u = energy[...]
    steps = jnp.where(active, CFL * h / jnp.sqrt(GAMMA * (GAMMA - 1.0) * u), 1e30)
    mine[...] = jnp.min(steps, axis=0, keepdims=True)

    wait_for = 3 + jnp.where(low, 1, 0) + jnp.where(high, 1, 0) + jnp.where(root, len(plane) + 1, 2)
    pl.semaphore_wait(barrier, wait_for)

    for zr in range(2):
        @pl.when(z != zr)
        def _():
            remote(mine, zbuf.at[pl.ds(z, 1)], msend.at[zr], mrecv.at[0], at(dom_of(zr, y, c), g)).start()

    for copy in loads[3:]:
        copy.wait()
    m = mass[...]

    own = (NG + g) * 4 * NB
    for comp in range(3):
        for b in range(NB):
            piece = pl.ds(b * W, W)
            rows[comp * NB + b : comp * NB + b + 1, :] = (
                pos[comp : comp + 1, piece] + DRIFT * vel[comp : comp + 1, piece]
            )
        pool[pl.ds(pl.multiple_of(own + comp * NB, NB), NB), :] = rows[comp * NB : comp * NB + NB, :]
    pool[pl.ds(pl.multiple_of(own + 3 * NB, NB), NB), :] = m
    pool[pl.ds(EMPTY * 4, 4 * NB), :] = jnp.zeros((4 * NB, W), jnp.float32)
    mfpool[pl.ds(EMPTY, NB), :] = jnp.zeros((NB, W), jnp.float32)
    res[pl.ds(4 * NB, NB), :] = jnp.zeros((NB, W), jnp.float32)

    targets = [tgt[b] for b in range(NB)]
    ranks = []
    for b in range(NB):
        r = jnp.int32(0)
        for e in range(b):
            r = r + jnp.where(targets[e] == targets[b], 1, 0)
        ranks.append(r)
    places = [targets[b] * CAP + ranks[b] for b in range(NB)]
    for s in range(NG * CAP):
        found = jnp.int32(NB)
        for b in range(NB):
            found = jnp.where(places[b] == s, b, found)
        table[NG + g, s] = found

    @pl.when(jnp.logical_not(low))
    def _():
        for d in range(NG):
            for s in range(NG * CAP):
                table[d, s] = jnp.int32(NB)

    @pl.when(jnp.logical_not(high))
    def _():
        for d in range(NG):
            for s in range(NG * CAP):
                table[2 * NG + d, s] = jnp.int32(NB)

    def piece_at(ref, per, i, d):
        return ref.at[pl.ds(pl.multiple_of((i * NG + lax.rem(g + d, NG)) * per, per), per)]

    def over_group(ref, per, send, recv, d):
        part = piece_at(ref, per, 1, 0)
        return remote(part, part, send.at[d], recv.at[NG - d], at(a, lax.rem(g + d, NG)))

    def to_side(ref, per, send, recv, d, up):
        src, dst = piece_at(ref, per, 1, d), piece_at(ref, per, 0 if up else 2, d)
        k = NG if up else NG + 1
        return remote(src, dst, send.at[(k - 3) * NG + d], recv.at[k], at(a + (1 if up else -1), g))

    def sides(parts, d, do):
        for up, there in ((True, high), (False, low)):
            @pl.when(there)
            def _():
                for part in parts:
                    do(to_side(*part, d, up))

    def gathered(parts, between):
        for d in (2, 1, 3):
            for part in parts:
                over_group(*part, d).start()
        sides(parts, 0, lambda copy: copy.start())
        between()
        for d in (1, 3, 2):
            for ref, per, send, recv in parts:
                landed(ref.at[pl.ds(0, per)], recv.at[d])
            sides(parts, d, lambda copy: copy.start())
        for k, there in ((NG, low), (NG + 1, high)):
            @pl.when(there)
            def _():
                for ref, per, send, recv in parts:
                    landed(ref.at[pl.ds(0, NG * per)], recv.at[k])

    def sent(parts):
        for d in (2, 1, 3):
            for part in parts:
                over_group(*part, d).wait_send()
        for d in range(NG):
            sides(parts, d, lambda copy: copy.wait_send())

    first = ((pool, 4 * NB, dsend, drecv), (table, 1, tsend, trecv))

    def columns():
        rows[3 * NB : 4 * NB, :] = h * h

        def one(b, _):
            for comp in range(4):
                row = rows[pl.ds(comp * NB + b, 1), :]
                cols[comp, pl.ds(pl.multiple_of(b * W, W), W), :] = jnp.transpose(jnp.broadcast_to(row, (W, W)))
            return 0

        lax.fori_loop(0, NB, one, 0)

    gathered(first, columns)

    def partner(b, k):
        if k == 0:
            return NG + g, b
        n = nbr[k - 1, b]
        cell, s = n // 16, n % 16
        i, j = cell // 3, cell % 3
        t = tgt[b] + j - 1
        d = i * NG + s // CAP
        e = table[d, jnp.clip(t, 0, NG - 1) * CAP + s % CAP]
        there = (t >= 0) & (t < NG) & (a + i >= 1) & (a + i <= n_dom) & (e < NB)
        return jnp.where(there, d, 3 * NG), jnp.where(there, e, 0)

    def find(b):
        who = [partner(b, k) for k in range(5)]
        for k, (d, e) in enumerate(who):
            base_of[b * 5 + k] = d * NB + e
        return who

    lane_of = lax.broadcasted_iota(jnp.int32, (CH, W), 1)

    def keep(q, b, sums):
        here = slice(q * CH, (q + 1) * CH)
        kept = coll[here, :]
        for k, s in enumerate(sums):
            kept = jnp.where(lane_of == k * NB + b, jnp.sum(s, axis=1, keepdims=True), kept)
        coll[here, :] = kept

    def stashed(b, k, q):
        return pl.ds(pl.multiple_of((b * 5 + k) * W + q * CH, CH), CH)

    def density_pairs(b, _):
        who = find(b)
        for q in range(W // CH):
            mine_at = pl.ds(pl.multiple_of(b * W + q * CH, CH), CH)
            cx, cy, cz, ch2 = (cols[comp, mine_at, :] for comp in range(4))
            sums = [jnp.zeros((CH, W), jnp.float32) for _ in range(4)]
            for k, (d, e) in enumerate(who):
                base = d * (4 * NB) + e
                dx = cx - pool[pl.ds(base, 1), :]
                dy = cy - pool[pl.ds(base + NB, 1), :]
                dz = cz - pool[pl.ds(base + 2 * NB, 1), :]
                w = jnp.maximum(ch2 - (dx * dx + dy * dy + dz * dz), 0.0)
                w2 = w * w
                m_j = pool[pl.ds(base + 3 * NB, 1), :]
                parts = []
                for comp, delta in enumerate((dx, dy, dz)):
                    part = w2 * delta
                    stash[comp, stashed(b, k, q), :] = part
                    parts.append(m_j * part)
                parts.append(m_j * (w2 * w))
                sums = [s + p for s, p in zip(sums, parts)]
            keep(q, b, sums)
        return 0

    def force_pairs(b, _):
        who = [base_of[b * 5 + k] for k in range(5)]
        for q in range(W // CH):
            sums = [jnp.zeros((CH, W), jnp.float32) for _ in range(3)]
            for k, base in enumerate(who):
                mf_j = mfpool[pl.ds(base, 1), :]
                sums = [s + mf_j * stash[comp, stashed(b, k, q), :] for comp, s in enumerate(sums)]
            keep(q, b, sums)
        return 0

    def pairs(block):
        coll[...] = jnp.zeros((W, W), jnp.float32)
        lax.fori_loop(0, NB, block, 0)
        return jnp.transpose(coll[...])

    inv_h = 1.0 / h
    ih3 = inv_h * inv_h * inv_h
    ih9 = KNORM * (ih3 * ih3 * ih3)

    found = pairs(density_pairs)
    rho = ih9 * found[3 * NB : 4 * NB, :]
    factor = (GAMMA - 1.0) * u / rho
    mfpool[pl.ds(pl.multiple_of((NG + g) * NB, NB), NB), :] = m * factor
    res[0:NB, :] = rho
    for comp in range(3):
        res[(1 + comp) * NB : (2 + comp) * NB, :] = factor * found[comp * NB : (comp + 1) * NB, :]

    part = mfpool.at[pl.ds(pl.multiple_of((NG + g) * NB, NB), NB)]

    def factors(i):
        dst = mfpool.at[pl.ds(pl.multiple_of(((1 - i) * NG + g) * NB, NB), NB)]
        to = others if i == 0 else others + [g]
        return [
            remote(part, dst, fsend.at[(i + 1) * NG + k], frecv.at[1 - i], at(a + i, o)) for k, o in enumerate(to)
        ]

    def on_sides(do):
        for i, there in ((1, high), (-1, low)):
            pl.when(there)(functools.partial(do, i))

    def start_factors(i):
        for copy in factors(i):
            copy.start()

    def sent_factors(i):
        for copy in factors(i):
            copy.wait_send()

    on_sides(start_factors)
    start_factors(0)
    landed(mfpool.at[pl.ds(0, 3 * NB)], frecv.at[1])
    on_sides(lambda i: landed(mfpool.at[pl.ds(0, NG * NB)], frecv.at[1 + i]))

    found = pairs(force_pairs)
    for comp in range(3):
        here = slice((1 + comp) * NB, (2 + comp) * NB)
        total = 6.0 * ih9 * (res[here, :] + found[comp * NB : (comp + 1) * NB, :])
        res[here, :] = jnp.where(active, total, 0.0)

    for t in range(NG):
        for r in range(CAP):
            e = table[NG + g, t * CAP + r]
            for comp in range(4):
                source = jnp.where(e < NB, comp * NB + e, 4 * NB)
                outsend[t, comp * CAP + r : comp * CAP + r + 1, :] = res[pl.ds(source, 1), :]
    results = [remote(outsend.at[o], outbuf.at[g], osend.at[k], orecv, at(a, o)) for k, o in enumerate(others)]
    for copy in results:
        copy.start()
    outbuf[g] = outsend[g]

    @pl.when(root)
    def _():
        zbuf[pl.ds(z, 1), :] = mine[...]
        landed(zbuf.at[pl.ds(0, NZ - 1)], mrecv.at[0])
        least = jnp.min(zbuf[...], axis=0, keepdims=True)
        index = (y * 2 + c) * NG + g
        last[...] = least
        xbuf[pl.ds(index, 1), :] = least
        for k, p in enumerate(plane):
            remote(last, xbuf.at[pl.ds(index, 1)], msend.at[2 + k], mrecv.at[1], p).start()

    landed(outbuf.at[pl.ds(0, 3)], orecv)
    slots_out[...] = outbuf[...]

    @pl.when(root)
    def _():
        landed(xbuf.at[pl.ds(0, len(plane))], mrecv.at[1])
        final[...] = jnp.min(xbuf[...], axis=0, keepdims=True)

        def child(k, _):
            to = jnp.where(z == 0, NZ - 1 - k, 2 + k)
            remote(final, final, msend.at[2 + len(plane) + k], mrecv.at[2], at(dom_of(to, y, c), g)).start()
            return 0

        lax.fori_loop(0, 7, child, 0)

    @pl.when(jnp.logical_not(root))
    def _():
        landed(final, mrecv.at[2])

    least_out[...] = final[...]

    sent(first)
    sent_factors(0)
    on_sides(sent_factors)
    for copy in results:
        copy.wait_send()
    for zr in range(2):
        @pl.when(z != zr)
        def _():
            landed(mine, msend.at[zr])

    @pl.when(root)
    def _():
        for k in range(len(plane) + 7):
            landed(last, msend.at[2 + k])


def unpack(slots_in, least_in, dens_out, acc_out, ts_out):
    for s in range(NG):
        dens_out[s * CAP : (s + 1) * CAP, :] = slots_in[s, 0:CAP, :]
        for comp in range(3):
            for r in range(CAP):
                row = (1 + comp) * CAP + r
                slot = s * CAP + r
                acc_out[comp : comp + 1, slot * W : (slot + 1) * W] = slots_in[s, row : row + 1, :]
    ts_out[0] = jnp.min(least_in[...])


def body(positions, velocity, smoothing, mass, energy, targets, neighbours, counts):
    f32 = jnp.float32
    slots = NG * CAP
    vmem, smem = pl.BlockSpec(memory_space=pltpu.VMEM), pl.BlockSpec(memory_space=pltpu.SMEM)
    sem = pltpu.SemaphoreType.DMA
    packed, least = pl.pallas_call(
        kernel,
        out_shape=(pltpu.VMEM((NG, 4 * CAP, W), f32), pltpu.VMEM((1, W), f32)),
        in_specs=[pl.BlockSpec(memory_space=pl.ANY)] * 8,
        out_specs=(vmem, vmem),
        scratch_shapes=[
            pltpu.SMEM((NB,), jnp.int32),
            pltpu.SMEM((4, NB), jnp.int32),
            pltpu.SMEM((NB,), jnp.int32),
            pltpu.VMEM((3, NB * W), f32),
            pltpu.VMEM((3, NB * W), f32),
            pltpu.VMEM((NB, W), f32),
            pltpu.VMEM((NB, W), f32),
            pltpu.VMEM((NB, W), f32),
            pltpu.SMEM((5 * NB,), jnp.int32),
            pltpu.VMEM(((EMPTY + NB) * 4, W), f32),
            pltpu.VMEM((EMPTY + NB, W), f32),
            pltpu.SMEM((3 * NG, 16), jnp.int32),
            pltpu.VMEM((4 * NB, W), f32),
            pltpu.VMEM((4, NB * W, W), f32),
            pltpu.VMEM((3, 5 * NB * W, W), f32),
            pltpu.VMEM((W, W), f32),
            pltpu.VMEM((5 * NB, W), f32),
            pltpu.VMEM((NG, 4 * CAP, W), f32),
            pltpu.VMEM((NG, 4 * CAP, W), f32),
            pltpu.VMEM((1, W), f32),
            pltpu.VMEM((NZ, W), f32),
            pltpu.VMEM((2 * NY * NG, W), f32),
            pltpu.VMEM((1, W), f32),
            pltpu.VMEM((1, W), f32),
            sem((8,)), sem((3 * NG,)), sem((6,)), sem((3 * NG,)), sem((6,)), sem((3 * NG,)), sem((3,)),
            sem((3,)), sem, sem((2 + 63 + 7,)), sem((3,)),
        ],
        compiler_params=pltpu.CompilerParams(collective_id=0, has_side_effects=True),
    )(
        targets.reshape(-1), neighbours.T, counts, positions, velocity,
        smoothing.reshape(NB, W), mass.reshape(NB, W), energy.reshape(NB, W),
    )
    dens, acc, ts = pl.pallas_call(
        unpack,
        out_shape=(
            jax.ShapeDtypeStruct((slots, W), f32),
            jax.ShapeDtypeStruct((3, slots * W), f32),
            jax.ShapeDtypeStruct((1,), f32),
        ),
        in_specs=[vmem] * 2,
        out_specs=(vmem, vmem, smem),
    )(*(pltpu.with_memory_space_constraint(v, pltpu.VMEM) for v in (packed, least)))
    return dens.reshape(-1), acc, ts


def solution(mesh):
    both = ("dom", "grp")
    return jax.shard_map(
        body,
        mesh=mesh,
        in_specs=(P(None, both), P(None, both), P(both), P(both), P(both), P(both, None), P(both, None), P(both)),
        out_specs=(P(both), P(None, both), P()),
        check_vma=False,
    )
```

```python
import functools
import math

import jax
import jax.numpy as jnp
from jax import lax
from jax.experimental import pallas as pl
from jax.experimental.pallas import tpu as pltpu
from jax.sharding import PartitionSpec as P

MESH = pl.DeviceIdType.MESH
CAP = 4
DRIFT = 0.05
GAMMA = 5.0 / 3.0
CFL = 0.3
KNORM = 315.0 / (64.0 * math.pi)

NB = 8
NG = 4
NZ, NY = 16, 8
W = 128
EMPTY = 12 * NB
CH = 32
ROOTS = (1, 2)


def at(dom, grp):
    return {"dom": dom, "grp": grp}


def remote(src, dst, send, recv, to):
    return pltpu.make_async_remote_copy(
        src_ref=src, dst_ref=dst, send_sem=send, recv_sem=recv, device_id=to, device_id_type=MESH
    )


def landed(ref, sem):
    pltpu.make_async_copy(ref, ref, sem).wait()


def kernel(
    tgt_in, nbr_in, cnt_in, pos_in, vel_in, smooth_in, mass_in, energy_in, slots_out, least_out,
    tgt, nbr, cnt, pos, vel, smooth, mass, energy, base_of,
    pool, mfpool, table, rows, cols, stash, coll, res, outsend, outbuf,
    mine, zbuf, xbuf, last, final,
    load, dsend, drecv, tsend, trecv, fsend, frecv, osend, orecv, msend, mrecv,
):
    a = lax.axis_index("dom")
    g = lax.axis_index("grp")
    n_dom = lax.axis_size("dom")
    z, y, c = a // 16, (a // 2) % 8, a % 2
    root = (z == ROOTS[0]) | (z == ROOTS[1])
    low, high = a > 0, a < n_dom - 1

    def dom_of(zz, yy, cc):
        return (zz * NY + yy) * 2 + cc

    others = [lax.rem(g + d, NG) for d in (2, 1, 3)]
    plane = [
        at(dom_of(z, lax.rem(y + dy, NY), lax.rem(c + dc, 2)), lax.rem(g + dx, NG))
        for dy in (4, 3, 5, 2, 6, 1, 7, 0) for dx in (2, 1, 3, 0) for dc in (0, 1) if dy or dx or dc
    ]

    loads = [
        pltpu.make_async_copy(src, dst, load.at[k])
        for k, (src, dst) in enumerate((
            (cnt_in, cnt), (smooth_in, smooth), (energy_in, energy), (tgt_in, tgt),
            (pos_in, pos), (vel_in, vel), (mass_in, mass), (nbr_in, nbr),
        ))
    ]
    for copy in loads:
        copy.start()

    barrier = pltpu.get_barrier_semaphore()

    def greet(to):
        pl.semaphore_signal(barrier, inc=1, device_id=to, device_id_type=MESH)

    for o in others:
        greet(at(a, o))

    @pl.when(low)
    def _():
        greet(at(a - 1, g))

    @pl.when(high)
    def _():
        greet(at(a + 1, g))

    @pl.when(root)
    def _():
        def child(k, _):
            greet(at(dom_of(lax.rem(ROOTS[1] + 1 + k, NZ), y, c), g))
            return 0

        lax.fori_loop(0, NZ - 2, child, 0)
        greet(at(dom_of(ROOTS[0] + ROOTS[1] - z, y, c), g))
        for p in plane:
            greet(p)

    lane = lax.broadcasted_iota(jnp.int32, (NB, W), 1)
    sub = lax.broadcasted_iota(jnp.int32, (NB, W), 0)
    for copy in loads[:3]:
        copy.wait()
    count = jnp.zeros((NB, W), jnp.int32)
    for b in range(NB):
        count = jnp.where(sub == b, cnt[b], count)
    active = lane < count
    h = smooth[...]
    u = energy[...]
    steps = jnp.where(active, CFL * h / jnp.sqrt(GAMMA * (GAMMA - 1.0) * u), 1e30)
    mine[...] = jnp.min(steps, axis=0, keepdims=True)

    wait_for = 3 + jnp.where(low, 1, 0) + jnp.where(high, 1, 0) + jnp.where(root, len(plane) + 1, 2)
    pl.semaphore_wait(barrier, wait_for)

    for k, zr in enumerate(ROOTS):
        @pl.when(z != zr)
        def _():
            remote(mine, zbuf.at[pl.ds(z, 1)], msend.at[k], mrecv.at[0], at(dom_of(zr, y, c), g)).start()

    for copy in loads[3:]:
        copy.wait()
    m = mass[...]

    own = (NG + g) * 4 * NB
    for comp in range(3):
        for b in range(NB):
            piece = pl.ds(b * W, W)
            rows[comp * NB + b : comp * NB + b + 1, :] = (
                pos[comp : comp + 1, piece] + DRIFT * vel[comp : comp + 1, piece]
            )
        pool[pl.ds(pl.multiple_of(own + comp * NB, NB), NB), :] = rows[comp * NB : comp * NB + NB, :]
    pool[pl.ds(pl.multiple_of(own + 3 * NB, NB), NB), :] = m
    pool[pl.ds(EMPTY * 4, 4 * NB), :] = jnp.zeros((4 * NB, W), jnp.float32)
    mfpool[pl.ds(EMPTY, NB), :] = jnp.zeros((NB, W), jnp.float32)
    res[pl.ds(4 * NB, NB), :] = jnp.zeros((NB, W), jnp.float32)

    targets = [tgt[b] for b in range(NB)]
    ranks = []
    for b in range(NB):
        r = jnp.int32(0)
        for e in range(b):
            r = r + jnp.where(targets[e] == targets[b], 1, 0)
        ranks.append(r)
    places = [targets[b] * CAP + ranks[b] for b in range(NB)]
    for s in range(NG * CAP):
        found = jnp.int32(NB)
        for b in range(NB):
            found = jnp.where(places[b] == s, b, found)
        table[NG + g, s] = found

    @pl.when(jnp.logical_not(low))
    def _():
        for d in range(NG):
            for s in range(NG * CAP):
                table[d, s] = jnp.int32(NB)

    @pl.when(jnp.logical_not(high))
    def _():
        for d in range(NG):
            for s in range(NG * CAP):
                table[2 * NG + d, s] = jnp.int32(NB)

    def piece_at(ref, per, i, d):
        return ref.at[pl.ds(pl.multiple_of((i * NG + lax.rem(g + d, NG)) * per, per), per)]

    def over_group(ref, per, send, recv, d):
        part = piece_at(ref, per, 1, 0)
        return remote(part, part, send.at[d], recv.at[NG - d], at(a, lax.rem(g + d, NG)))

    def to_side(ref, per, send, recv, d, up):
        src, dst = piece_at(ref, per, 1, d), piece_at(ref, per, 0 if up else 2, d)
        k = NG if up else NG + 1
        return remote(src, dst, send.at[(k - 3) * NG + d], recv.at[k], at(a + (1 if up else -1), g))

    def sides(parts, d, do):
        for up, there in ((True, high), (False, low)):
            @pl.when(there)
            def _():
                for part in parts:
                    do(to_side(*part, d, up))

    def gathered(parts, between):
        for d in (2, 1, 3):
            for part in parts:
                over_group(*part, d).start()
        sides(parts, 0, lambda copy: copy.start())
        between()
        for d in (1, 3, 2):
            for ref, per, send, recv in parts:
                landed(ref.at[pl.ds(0, per)], recv.at[d])
            sides(parts, d, lambda copy: copy.start())
        for k, there in ((NG, low), (NG + 1, high)):
            @pl.when(there)
            def _():
                for ref, per, send, recv in parts:
                    landed(ref.at[pl.ds(0, NG * per)], recv.at[k])

    def sent(parts):
        for d in (2, 1, 3):
            for part in parts:
                over_group(*part, d).wait_send()
        for d in range(NG):
            sides(parts, d, lambda copy: copy.wait_send())

    first = ((pool, 4 * NB, dsend, drecv), (table, 1, tsend, trecv))

    def columns():
        rows[3 * NB : 4 * NB, :] = h * h

        def one(b, _):
            for comp in range(4):
                row = rows[pl.ds(comp * NB + b, 1), :]
                cols[comp, pl.ds(pl.multiple_of(b * W, W), W), :] = jnp.transpose(jnp.broadcast_to(row, (W, W)))
            return 0

        lax.fori_loop(0, NB, one, 0)

    gathered(first, columns)

    def partner(b, k):
        if k == 0:
            return NG + g, b
        n = nbr[k - 1, b]
        cell, s = n // 16, n % 16
        i, j = cell // 3, cell % 3
        t = tgt[b] + j - 1
        d = i * NG + s // CAP
        e = table[d, jnp.clip(t, 0, NG - 1) * CAP + s % CAP]
        there = (t >= 0) & (t < NG) & (a + i >= 1) & (a + i <= n_dom) & (e < NB)
        return jnp.where(there, d, 3 * NG), jnp.where(there, e, 0)

    def find(b):
        who = [partner(b, k) for k in range(5)]
        for k, (d, e) in enumerate(who):
            base_of[b * 5 + k] = d * NB + e
        return who

    lane_of = lax.broadcasted_iota(jnp.int32, (CH, W), 1)

    def keep(q, b, sums):
        here = slice(q * CH, (q + 1) * CH)
        kept = coll[here, :]
        for k, s in enumerate(sums):
            kept = jnp.where(lane_of == k * NB + b, jnp.sum(s, axis=1, keepdims=True), kept)
        coll[here, :] = kept

    def stashed(b, k, q):
        return pl.ds(pl.multiple_of((b * 5 + k) * W + q * CH, CH), CH)

    def density_pairs(b, _):
        who = find(b)
        for q in range(W // CH):
            mine_at = pl.ds(pl.multiple_of(b * W + q * CH, CH), CH)
            cx, cy, cz, ch2 = (cols[comp, mine_at, :] for comp in range(4))
            sums = [jnp.zeros((CH, W), jnp.float32) for _ in range(4)]
            for k, (d, e) in enumerate(who):
                base = d * (4 * NB) + e
                dx = cx - pool[pl.ds(base, 1), :]
                dy = cy - pool[pl.ds(base + NB, 1), :]
                dz = cz - pool[pl.ds(base + 2 * NB, 1), :]
                w = jnp.maximum(ch2 - (dx * dx + dy * dy + dz * dz), 0.0)
                w2 = w * w
                m_j = pool[pl.ds(base + 3 * NB, 1), :]
                parts = []
                for comp, delta in enumerate((dx, dy, dz)):
                    part = w2 * delta
                    stash[comp, stashed(b, k, q), :] = part
                    parts.append(m_j * part)
                parts.append(m_j * (w2 * w))
                sums = [s + p for s, p in zip(sums, parts)]
            keep(q, b, sums)
        return 0

    def force_pairs(b, _):
        who = [base_of[b * 5 + k] for k in range(5)]
        for q in range(W // CH):
            sums = [jnp.zeros((CH, W), jnp.float32) for _ in range(3)]
            for k, base in enumerate(who):
                mf_j = mfpool[pl.ds(base, 1), :]
                sums = [s + mf_j * stash[comp, stashed(b, k, q), :] for comp, s in enumerate(sums)]
            keep(q, b, sums)
        return 0

    def pairs(block):
        coll[...] = jnp.zeros((W, W), jnp.float32)
        lax.fori_loop(0, NB, block, 0)
        return jnp.transpose(coll[...])

    inv_h = 1.0 / h
    ih3 = inv_h * inv_h * inv_h
    ih9 = KNORM * (ih3 * ih3 * ih3)

    found = pairs(density_pairs)
    rho = ih9 * found[3 * NB : 4 * NB, :]
    factor = (GAMMA - 1.0) * u / rho
    mfpool[pl.ds(pl.multiple_of((NG + g) * NB, NB), NB), :] = m * factor
    res[0:NB, :] = rho
    for comp in range(3):
        res[(1 + comp) * NB : (2 + comp) * NB, :] = factor * found[comp * NB : (comp + 1) * NB, :]

    part = mfpool.at[pl.ds(pl.multiple_of((NG + g) * NB, NB), NB)]

    def factors(i):
        dst = mfpool.at[pl.ds(pl.multiple_of(((1 - i) * NG + g) * NB, NB), NB)]
        to = others if i == 0 else others + [g]
        return [
            remote(part, dst, fsend.at[(i + 1) * NG + k], frecv.at[1 - i], at(a + i, o)) for k, o in enumerate(to)
        ]

    def on_sides(do):
        for i, there in ((1, high), (-1, low)):
            pl.when(there)(functools.partial(do, i))

    def start_factors(i):
        for copy in factors(i):
            copy.start()

    def sent_factors(i):
        for copy in factors(i):
            copy.wait_send()

    on_sides(start_factors)
    start_factors(0)
    landed(mfpool.at[pl.ds(0, 3 * NB)], frecv.at[1])
    on_sides(lambda i: landed(mfpool.at[pl.ds(0, NG * NB)], frecv.at[1 + i]))

    found = pairs(force_pairs)
    for comp in range(3):
        here = slice((1 + comp) * NB, (2 + comp) * NB)
        total = 6.0 * ih9 * (res[here, :] + found[comp * NB : (comp + 1) * NB, :])
        res[here, :] = jnp.where(active, total, 0.0)

    for t in range(NG):
        for r in range(CAP):
            e = table[NG + g, t * CAP + r]
            for comp in range(4):
                source = jnp.where(e < NB, comp * NB + e, 4 * NB)
                outsend[t, comp * CAP + r : comp * CAP + r + 1, :] = res[pl.ds(source, 1), :]
    results = [remote(outsend.at[o], outbuf.at[g], osend.at[k], orecv, at(a, o)) for k, o in enumerate(others)]
    for copy in results:
        copy.start()
    outbuf[g] = outsend[g]

    @pl.when(root)
    def _():
        zbuf[pl.ds(z, 1), :] = mine[...]
        landed(zbuf.at[pl.ds(0, NZ - 1)], mrecv.at[0])
        least = jnp.min(zbuf[...], axis=0, keepdims=True)
        index = (y * 2 + c) * NG + g
        last[...] = least
        xbuf[pl.ds(index, 1), :] = least
        for k, p in enumerate(plane):
            remote(last, xbuf.at[pl.ds(index, 1)], msend.at[2 + k], mrecv.at[1], p).start()

    landed(outbuf.at[pl.ds(0, 3)], orecv)
    slots_out[...] = outbuf[...]

    @pl.when(root)
    def _():
        landed(xbuf.at[pl.ds(0, len(plane))], mrecv.at[1])
        final[...] = jnp.min(xbuf[...], axis=0, keepdims=True)

        def child(k, _):
            to = jnp.where(z == ROOTS[0], lax.rem(ROOTS[0] + NZ - 1 - k, NZ), lax.rem(ROOTS[1] + 1 + k, NZ))
            remote(final, final, msend.at[2 + len(plane) + k], mrecv.at[2], at(dom_of(to, y, c), g)).start()
            return 0

        lax.fori_loop(0, 7, child, 0)

    @pl.when(jnp.logical_not(root))
    def _():
        landed(final, mrecv.at[2])

    least_out[...] = final[...]

    sent(first)
    sent_factors(0)
    on_sides(sent_factors)
    for copy in results:
        copy.wait_send()
    for k, zr in enumerate(ROOTS):
        @pl.when(z != zr)
        def _():
            landed(mine, msend.at[k])

    @pl.when(root)
    def _():
        for k in range(len(plane) + 7):
            landed(last, msend.at[2 + k])


def unpack(slots_in, least_in, dens_out, acc_out, ts_out):
    for s in range(NG):
        dens_out[s * CAP : (s + 1) * CAP, :] = slots_in[s, 0:CAP, :]
        for comp in range(3):
            for r in range(CAP):
                row = (1 + comp) * CAP + r
                slot = s * CAP + r
                acc_out[comp : comp + 1, slot * W : (slot + 1) * W] = slots_in[s, row : row + 1, :]
    ts_out[0] = jnp.min(least_in[...])


def body(positions, velocity, smoothing, mass, energy, targets, neighbours, counts):
    f32 = jnp.float32
    slots = NG * CAP
    vmem, smem = pl.BlockSpec(memory_space=pltpu.VMEM), pl.BlockSpec(memory_space=pltpu.SMEM)
    sem = pltpu.SemaphoreType.DMA
    packed, least = pl.pallas_call(
        kernel,
        out_shape=(pltpu.VMEM((NG, 4 * CAP, W), f32), pltpu.VMEM((1, W), f32)),
        in_specs=[pl.BlockSpec(memory_space=pl.ANY)] * 8,
        out_specs=(vmem, vmem),
        scratch_shapes=[
            pltpu.SMEM((NB,), jnp.int32),
            pltpu.SMEM((4, NB), jnp.int32),
            pltpu.SMEM((NB,), jnp.int32),
            pltpu.VMEM((3, NB * W), f32),
            pltpu.VMEM((3, NB * W), f32),
            pltpu.VMEM((NB, W), f32),
            pltpu.VMEM((NB, W), f32),
            pltpu.VMEM((NB, W), f32),
            pltpu.SMEM((5 * NB,), jnp.int32),
            pltpu.VMEM(((EMPTY + NB) * 4, W), f32),
            pltpu.VMEM((EMPTY + NB, W), f32),
            pltpu.SMEM((3 * NG, 16), jnp.int32),
            pltpu.VMEM((4 * NB, W), f32),
            pltpu.VMEM((4, NB * W, W), f32),
            pltpu.VMEM((3, 5 * NB * W, W), f32),
            pltpu.VMEM((W, W), f32),
            pltpu.VMEM((5 * NB, W), f32),
            pltpu.VMEM((NG, 4 * CAP, W), f32),
            pltpu.VMEM((NG, 4 * CAP, W), f32),
            pltpu.VMEM((1, W), f32),
            pltpu.VMEM((NZ, W), f32),
            pltpu.VMEM((2 * NY * NG, W), f32),
            pltpu.VMEM((1, W), f32),
            pltpu.VMEM((1, W), f32),
            sem((8,)), sem((3 * NG,)), sem((6,)), sem((3 * NG,)), sem((6,)), sem((3 * NG,)), sem((3,)),
            sem((3,)), sem, sem((2 + 63 + 7,)), sem((3,)),
        ],
        compiler_params=pltpu.CompilerParams(collective_id=0, has_side_effects=True),
    )(
        targets.reshape(-1), neighbours.T, counts, positions, velocity,
        smoothing.reshape(NB, W), mass.reshape(NB, W), energy.reshape(NB, W),
    )
    dens, acc, ts = pl.pallas_call(
        unpack,
        out_shape=(
            jax.ShapeDtypeStruct((slots, W), f32),
            jax.ShapeDtypeStruct((3, slots * W), f32),
            jax.ShapeDtypeStruct((1,), f32),
        ),
        in_specs=[vmem] * 2,
        out_specs=(vmem, vmem, smem),
    )(*(pltpu.with_memory_space_constraint(v, pltpu.VMEM) for v in (packed, least)))
    return dens.reshape(-1), acc, ts


def solution(mesh):
    both = ("dom", "grp")
    return jax.shard_map(
        body,
        mesh=mesh,
        in_specs=(P(None, both), P(None, both), P(both), P(both), P(both), P(both, None), P(both, None), P(both)),
        out_specs=(P(both), P(None, both), P()),
        check_vma=False,
    )
```

```python
import functools
import math

import jax
import jax.numpy as jnp
from jax import lax
from jax.experimental import pallas as pl
from jax.experimental.pallas import tpu as pltpu
from jax.sharding import PartitionSpec as P

MESH = pl.DeviceIdType.MESH
CAP = 4
DRIFT = 0.05
GAMMA = 5.0 / 3.0
CFL = 0.3
KNORM = 315.0 / (64.0 * math.pi)

NB = 8
NG = 4
NZ, NY = 16, 8
W = 128
EMPTY = 12 * NB
CH = 32


def at(dom, grp):
    return {"dom": dom, "grp": grp}


def remote(src, dst, send, recv, to):
    return pltpu.make_async_remote_copy(
        src_ref=src, dst_ref=dst, send_sem=send, recv_sem=recv, device_id=to, device_id_type=MESH
    )


def landed(ref, sem):
    pltpu.make_async_copy(ref, ref, sem).wait()


def kernel(
    tgt_in, nbr_in, cnt_in, pos_in, vel_in, smooth_in, mass_in, energy_in, slots_out, least_out,
    tgt, nbr, cnt, pos, vel, smooth, mass, energy, base_of,
    pool, mfpool, table, rows, cols, stash, coll, res, outsend, outbuf,
    mine, zbuf, xbuf, last, final,
    load, dsend, drecv, tsend, trecv, fsend, frecv, osend, orecv, msend, mrecv,
):
    a = lax.axis_index("dom")
    g = lax.axis_index("grp")
    n_dom = lax.axis_size("dom")
    z, y, c = a // 16, (a // 2) % 8, a % 2
    column = (y == 0) & (c == 0) & (g == 0)
    zeroth = column & (z == 0)
    stand_in = (a == 1) & (g == 0)
    root = (z < 2) & jnp.logical_not(zeroth)
    children = jnp.where(column, NZ - 1, 7)
    low, high = a > 0, a < n_dom - 1

    def dom_of(zz, yy, cc):
        return (zz * NY + yy) * 2 + cc

    others = [lax.rem(g + d, NG) for d in (2, 1, 3)]
    moves = [(dy, dx, dc) for dy in (4, 3, 5, 2, 6, 1, 7, 0) for dx in (2, 1, 3, 0) for dc in (0, 1) if dy or dx or dc]

    def with_plane(do):
        for k, (dy, dx, dc) in enumerate(moves):
            dom, grp = dom_of(z, lax.rem(y + dy, NY), lax.rem(c + dc, 2)), lax.rem(g + dx, NG)
            pl.when((dom > 0) | (grp > 0))(functools.partial(do, k, at(dom, grp)))

    loads = [
        pltpu.make_async_copy(src, dst, load.at[k])
        for k, (src, dst) in enumerate((
            (cnt_in, cnt), (smooth_in, smooth), (energy_in, energy), (tgt_in, tgt),
            (pos_in, pos), (vel_in, vel), (mass_in, mass), (nbr_in, nbr),
        ))
    ]
    for copy in loads:
        copy.start()

    barrier = pltpu.get_barrier_semaphore()

    def greet(to):
        pl.semaphore_signal(barrier, inc=1, device_id=to, device_id_type=MESH)

    for o in others:
        greet(at(a, o))

    @pl.when(low)
    def _():
        greet(at(a - 1, g))

    @pl.when(high)
    def _():
        greet(at(a + 1, g))

    @pl.when(root)
    def _():
        def child(k, _):
            greet(at(dom_of(lax.rem(z + 1 + k, NZ), y, c), g))
            return 0

        lax.fori_loop(0, NZ - 1, child, 0)
        with_plane(lambda k, p: greet(p))

    @pl.when(stand_in)
    def _():
        def child(k, _):
            greet(at(dom_of(k, 0, 0), 0))
            return 0

        lax.fori_loop(0, NZ, child, 0)

    lane = lax.broadcasted_iota(jnp.int32, (NB, W), 1)
    sub = lax.broadcasted_iota(jnp.int32, (NB, W), 0)
    for copy in loads[:3]:
        copy.wait()
    count = jnp.zeros((NB, W), jnp.int32)
    for b in range(NB):
        count = jnp.where(sub == b, cnt[b], count)
    active = lane < count
    h = smooth[...]
    u = energy[...]
    steps = jnp.where(active, CFL * h / jnp.sqrt(GAMMA * (GAMMA - 1.0) * u), 1e30)
    mine[...] = jnp.min(steps, axis=0, keepdims=True)

    wait_for = 3 + jnp.where(low, 1, 0) + jnp.where(high, 1, 0) + jnp.where(root, jnp.where(z == 0, len(moves), len(moves) + 1), 2)
    pl.semaphore_wait(barrier, wait_for)

    def report(zr):
        to, row = dom_of(zr, y, c), z
        if zr == 0:
            to, row = jnp.where(column, 1, to), jnp.where(column, NZ + z, z)
        return remote(mine, zbuf.at[pl.ds(row, 1)], msend.at[zr], mrecv.at[0], at(to, g))

    reports = ((0, (z > 0) | zeroth), (1, z != 1))
    for zr, there in reports:
        pl.when(there)(lambda zr=zr: report(zr).start())

    @pl.when(root & jnp.logical_not(stand_in))
    def _():
        zbuf[NZ : 2 * NZ, :] = jnp.full((NZ, W), 1e30, jnp.float32)

    @pl.when(root & (z == 0))
    def _():
        xbuf[0:1, :] = jnp.full((1, W), 1e30, jnp.float32)

    for copy in loads[3:]:
        copy.wait()
    m = mass[...]

    own = (NG + g) * 4 * NB
    for comp in range(3):
        for b in range(NB):
            piece = pl.ds(b * W, W)
            rows[comp * NB + b : comp * NB + b + 1, :] = (
                pos[comp : comp + 1, piece] + DRIFT * vel[comp : comp + 1, piece]
            )
        pool[pl.ds(pl.multiple_of(own + comp * NB, NB), NB), :] = rows[comp * NB : comp * NB + NB, :]
    pool[pl.ds(pl.multiple_of(own + 3 * NB, NB), NB), :] = m
    pool[pl.ds(EMPTY * 4, 4 * NB), :] = jnp.zeros((4 * NB, W), jnp.float32)
    mfpool[pl.ds(EMPTY, NB), :] = jnp.zeros((NB, W), jnp.float32)
    res[pl.ds(4 * NB, NB), :] = jnp.zeros((NB, W), jnp.float32)

    targets = [tgt[b] for b in range(NB)]
    ranks = []
    for b in range(NB):
        r = jnp.int32(0)
        for e in range(b):
            r = r + jnp.where(targets[e] == targets[b], 1, 0)
        ranks.append(r)
    places = [targets[b] * CAP + ranks[b] for b in range(NB)]
    for s in range(NG * CAP):
        found = jnp.int32(NB)
        for b in range(NB):
            found = jnp.where(places[b] == s, b, found)
        table[NG + g, s] = found

    @pl.when(jnp.logical_not(low))
    def _():
        for d in range(NG):
            for s in range(NG * CAP):
                table[d, s] = jnp.int32(NB)

    @pl.when(jnp.logical_not(high))
    def _():
        for d in range(NG):
            for s in range(NG * CAP):
                table[2 * NG + d, s] = jnp.int32(NB)

    def piece_at(ref, per, i, d):
        return ref.at[pl.ds(pl.multiple_of((i * NG + lax.rem(g + d, NG)) * per, per), per)]

    def over_group(ref, per, send, recv, d):
        part = piece_at(ref, per, 1, 0)
        return remote(part, part, send.at[d], recv.at[NG - d], at(a, lax.rem(g + d, NG)))

    def to_side(ref, per, send, recv, d, up):
        src, dst = piece_at(ref, per, 1, d), piece_at(ref, per, 0 if up else 2, d)
        k = NG if up else NG + 1
        return remote(src, dst, send.at[(k - 3) * NG + d], recv.at[k], at(a + (1 if up else -1), g))

    def sides(parts, d, do):
        for up, there in ((True, high), (False, low)):
            @pl.when(there)
            def _():
                for part in parts:
                    do(to_side(*part, d, up))

    def gathered(parts, between):
        for d in (2, 1, 3):
            for part in parts:
                over_group(*part, d).start()
        sides(parts, 0, lambda copy: copy.start())
        between()
        for d in (1, 3, 2):
            for ref, per, send, recv in parts:
                landed(ref.at[pl.ds(0, per)], recv.at[d])
            sides(parts, d, lambda copy: copy.start())
        for k, there in ((NG, low), (NG + 1, high)):
            @pl.when(there)
            def _():
                for ref, per, send, recv in parts:
                    landed(ref.at[pl.ds(0, NG * per)], recv.at[k])

    def sent(parts):
        for d in (2, 1, 3):
            for part in parts:
                over_group(*part, d).wait_send()
        for d in range(NG):
            sides(parts, d, lambda copy: copy.wait_send())

    first = ((pool, 4 * NB, dsend, drecv), (table, 1, tsend, trecv))

    def columns():
        rows[3 * NB : 4 * NB, :] = h * h

        def one(b, _):
            for comp in range(4):
                row = rows[pl.ds(comp * NB + b, 1), :]
                cols[comp, pl.ds(pl.multiple_of(b * W, W), W), :] = jnp.transpose(jnp.broadcast_to(row, (W, W)))
            return 0

        lax.fori_loop(0, NB, one, 0)

    gathered(first, columns)

    def partner(b, k):
        if k == 0:
            return NG + g, b
        n = nbr[k - 1, b]
        cell, s = n // 16, n % 16
        i, j = cell // 3, cell % 3
        t = tgt[b] + j - 1
        d = i * NG + s // CAP
        e = table[d, jnp.clip(t, 0, NG - 1) * CAP + s % CAP]
        there = (t >= 0) & (t < NG) & (a + i >= 1) & (a + i <= n_dom) & (e < NB)
        return jnp.where(there, d, 3 * NG), jnp.where(there, e, 0)

    def find(b):
        who = [partner(b, k) for k in range(5)]
        for k, (d, e) in enumerate(who):
            base_of[b * 5 + k] = d * NB + e
        return who

    lane_of = lax.broadcasted_iota(jnp.int32, (CH, W), 1)

    def keep(q, b, sums):
        here = slice(q * CH, (q + 1) * CH)
        kept = coll[here, :]
        for k, s in enumerate(sums):
            kept = jnp.where(lane_of == k * NB + b, jnp.sum(s, axis=1, keepdims=True), kept)
        coll[here, :] = kept

    def stashed(b, k, q):
        return pl.ds(pl.multiple_of((b * 5 + k) * W + q * CH, CH), CH)

    def density_pairs(b, _):
        who = find(b)
        for q in range(W // CH):
            mine_at = pl.ds(pl.multiple_of(b * W + q * CH, CH), CH)
            cx, cy, cz, ch2 = (cols[comp, mine_at, :] for comp in range(4))
            sums = [jnp.zeros((CH, W), jnp.float32) for _ in range(4)]
            for k, (d, e) in enumerate(who):
                base = d * (4 * NB) + e
                dx = cx - pool[pl.ds(base, 1), :]
                dy = cy - pool[pl.ds(base + NB, 1), :]
                dz = cz - pool[pl.ds(base + 2 * NB, 1), :]
                w = jnp.maximum(ch2 - (dx * dx + dy * dy + dz * dz), 0.0)
                w2 = w * w
                m_j = pool[pl.ds(base + 3 * NB, 1), :]
                parts = []
                for comp, delta in enumerate((dx, dy, dz)):
                    part = w2 * delta
                    stash[comp, stashed(b, k, q), :] = part
                    parts.append(m_j * part)
                parts.append(m_j * (w2 * w))
                sums = [s + p for s, p in zip(sums, parts)]
            keep(q, b, sums)
        return 0

    def force_pairs(b, _):
        who = [base_of[b * 5 + k] for k in range(5)]
        for q in range(W // CH):
            sums = [jnp.zeros((CH, W), jnp.float32) for _ in range(3)]
            for k, base in enumerate(who):
                mf_j = mfpool[pl.ds(base, 1), :]
                sums = [s + mf_j * stash[comp, stashed(b, k, q), :] for comp, s in enumerate(sums)]
            keep(q, b, sums)
        return 0

    def pairs(block):
        coll[...] = jnp.zeros((W, W), jnp.float32)
        def two(b, _):
            block(2 * b, 0)
            block(2 * b + 1, 0)
            return 0

        lax.fori_loop(0, NB // 2, two, 0)
        return jnp.transpose(coll[...])

    inv_h = 1.0 / h
    ih3 = inv_h * inv_h * inv_h
    ih9 = KNORM * (ih3 * ih3 * ih3)

    found = pairs(density_pairs)
    rho = ih9 * found[3 * NB : 4 * NB, :]
    factor = (GAMMA - 1.0) * u / rho
    mfpool[pl.ds(pl.multiple_of((NG + g) * NB, NB), NB), :] = m * factor
    res[0:NB, :] = rho
    for comp in range(3):
        res[(1 + comp) * NB : (2 + comp) * NB, :] = factor * found[comp * NB : (comp + 1) * NB, :]

    part = mfpool.at[pl.ds(pl.multiple_of((NG + g) * NB, NB), NB)]

    def factors(i):
        dst = mfpool.at[pl.ds(pl.multiple_of(((1 - i) * NG + g) * NB, NB), NB)]
        to = others if i == 0 else others + [g]
        return [
            remote(part, dst, fsend.at[(i + 1) * NG + k], frecv.at[1 - i], at(a + i, o)) for k, o in enumerate(to)
        ]

    def on_sides(do):
        for i, there in ((1, high), (-1, low)):
            pl.when(there)(functools.partial(do, i))

    def start_factors(i):
        for copy in factors(i):
            copy.start()

    def sent_factors(i):
        for copy in factors(i):
            copy.wait_send()

    on_sides(start_factors)
    start_factors(0)
    landed(mfpool.at[pl.ds(0, 3 * NB)], frecv.at[1])
    on_sides(lambda i: landed(mfpool.at[pl.ds(0, NG * NB)], frecv.at[1 + i]))

    found = pairs(force_pairs)
    for comp in range(3):
        here = slice((1 + comp) * NB, (2 + comp) * NB)
        total = 6.0 * ih9 * (res[here, :] + found[comp * NB : (comp + 1) * NB, :])
        res[here, :] = jnp.where(active, total, 0.0)

    for t in range(NG):
        for r in range(CAP):
            e = table[NG + g, t * CAP + r]
            for comp in range(4):
                source = jnp.where(e < NB, comp * NB + e, 4 * NB)
                outsend[t, comp * CAP + r : comp * CAP + r + 1, :] = res[pl.ds(source, 1), :]
    results = [remote(outsend.at[o], outbuf.at[g], osend.at[k], orecv, at(a, o)) for k, o in enumerate(others)]
    for copy in results:
        copy.start()
    outbuf[g] = outsend[g]

    @pl.when(root)
    def _():
        zbuf[pl.ds(z, 1), :] = mine[...]

        @pl.when(stand_in)
        def _():
            landed(zbuf.at[pl.ds(0, 2 * NZ - 1)], mrecv.at[0])

        @pl.when(jnp.logical_not(stand_in))
        def _():
            landed(zbuf.at[pl.ds(0, NZ - 1)], mrecv.at[0])

        least = jnp.min(zbuf[...], axis=0, keepdims=True)
        index = (y * 2 + c) * NG + g
        last[...] = least
        xbuf[pl.ds(index, 1), :] = least
        with_plane(lambda k, p: remote(last, xbuf.at[pl.ds(index, 1)], msend.at[2 + k], mrecv.at[1], p).start())

    landed(outbuf.at[pl.ds(0, 3)], orecv)
    slots_out[...] = outbuf[...]

    @pl.when(root)
    def _():
        @pl.when(z == 0)
        def _():
            landed(xbuf.at[pl.ds(0, len(moves) - 1)], mrecv.at[1])

        @pl.when(z != 0)
        def _():
            landed(xbuf.at[pl.ds(0, len(moves))], mrecv.at[1])

        final[...] = jnp.min(xbuf[...], axis=0, keepdims=True)

        def child(k, _):
            to = jnp.where(z == 0, NZ - 1 - k, lax.rem(2 + k, NZ))
            remote(final, final, msend.at[65 + k], mrecv.at[2], at(dom_of(to, y, c), g)).start()
            return 0

        lax.fori_loop(0, children, child, 0)

    @pl.when(jnp.logical_not(root))
    def _():
        landed(final, mrecv.at[2])

    least_out[...] = final[...]

    sent(first)
    sent_factors(0)
    on_sides(sent_factors)
    for copy in results:
        copy.wait_send()
    for zr, there in reports:
        pl.when(there)(lambda zr=zr: report(zr).wait_send())

    @pl.when(root)
    def _():
        with_plane(lambda k, p: landed(last, msend.at[2 + k]))

        def child(k, _):
            landed(last, msend.at[65 + k])
            return 0

        lax.fori_loop(0, children, child, 0)


def unpack(slots_in, least_in, dens_out, acc_out, ts_out):
    for s in range(NG):
        dens_out[s * CAP : (s + 1) * CAP, :] = slots_in[s, 0:CAP, :]
        for comp in range(3):
            for r in range(CAP):
                row = (1 + comp) * CAP + r
                slot = s * CAP + r
                acc_out[comp : comp + 1, slot * W : (slot + 1) * W] = slots_in[s, row : row + 1, :]
    ts_out[0] = jnp.min(least_in[...])


def body(positions, velocity, smoothing, mass, energy, targets, neighbours, counts):
    f32 = jnp.float32
    slots = NG * CAP
    vmem, smem = pl.BlockSpec(memory_space=pltpu.VMEM), pl.BlockSpec(memory_space=pltpu.SMEM)
    sem = pltpu.SemaphoreType.DMA
    packed, least = pl.pallas_call(
        kernel,
        out_shape=(pltpu.VMEM((NG, 4 * CAP, W), f32), pltpu.VMEM((1, W), f32)),
        in_specs=[pl.BlockSpec(memory_space=pl.ANY)] * 8,
        out_specs=(vmem, vmem),
        scratch_shapes=[
            pltpu.SMEM((NB,), jnp.int32),
            pltpu.SMEM((4, NB), jnp.int32),
            pltpu.SMEM((NB,), jnp.int32),
            pltpu.VMEM((3, NB * W), f32),
            pltpu.VMEM((3, NB * W), f32),
            pltpu.VMEM((NB, W), f32),
            pltpu.VMEM((NB, W), f32),
            pltpu.VMEM((NB, W), f32),
            pltpu.SMEM((5 * NB,), jnp.int32),
            pltpu.VMEM(((EMPTY + NB) * 4, W), f32),
            pltpu.VMEM((EMPTY + NB, W), f32),
            pltpu.SMEM((3 * NG, 16), jnp.int32),
            pltpu.VMEM((4 * NB, W), f32),
            pltpu.VMEM((4, NB * W, W), f32),
            pltpu.VMEM((3, 5 * NB * W, W), f32),
            pltpu.VMEM((W, W), f32),
            pltpu.VMEM((5 * NB, W), f32),
            pltpu.VMEM((NG, 4 * CAP, W), f32),
            pltpu.VMEM((NG, 4 * CAP, W), f32),
            pltpu.VMEM((1, W), f32),
            pltpu.VMEM((2 * NZ, W), f32),
            pltpu.VMEM((2 * NY * NG, W), f32),
            pltpu.VMEM((1, W), f32),
            pltpu.VMEM((1, W), f32),
            sem((8,)), sem((3 * NG,)), sem((6,)), sem((3 * NG,)), sem((6,)), sem((3 * NG,)), sem((3,)),
            sem((3,)), sem, sem((2 + 63 + 15,)), sem((3,)),
        ],
        compiler_params=pltpu.CompilerParams(collective_id=0, has_side_effects=True),
    )(
        targets.reshape(-1), neighbours.T, counts, positions, velocity,
        smoothing.reshape(NB, W), mass.reshape(NB, W), energy.reshape(NB, W),
    )
    dens, acc, ts = pl.pallas_call(
        unpack,
        out_shape=(
            jax.ShapeDtypeStruct((slots, W), f32),
            jax.ShapeDtypeStruct((3, slots * W), f32),
            jax.ShapeDtypeStruct((1,), f32),
        ),
        in_specs=[vmem] * 2,
        out_specs=(vmem, vmem, smem),
    )(*(pltpu.with_memory_space_constraint(v, pltpu.VMEM) for v in (packed, least)))
    return dens.reshape(-1), acc, ts


def solution(mesh):
    both = ("dom", "grp")
    return jax.shard_map(
        body,
        mesh=mesh,
        in_specs=(P(None, both), P(None, both), P(both), P(both), P(both), P(both, None), P(both, None), P(both)),
        out_specs=(P(both), P(None, both), P()),
        check_vma=False,
    )
```

```python
import functools
import math

import jax
import jax.numpy as jnp
from jax import lax
from jax.experimental import pallas as pl
from jax.experimental.pallas import tpu as pltpu
from jax.sharding import PartitionSpec as P

MESH = pl.DeviceIdType.MESH
CAP = 4
DRIFT = 0.05
GAMMA = 5.0 / 3.0
CFL = 0.3
KNORM = 315.0 / (64.0 * math.pi)

NB = 8
NG = 4
NZ, NY = 16, 8
W = 128
EMPTY = 12 * NB
CH = 32


def at(dom, grp):
    return {"dom": dom, "grp": grp}


def remote(src, dst, send, recv, to):
    return pltpu.make_async_remote_copy(
        src_ref=src, dst_ref=dst, send_sem=send, recv_sem=recv, device_id=to, device_id_type=MESH
    )


def landed(ref, sem):
    pltpu.make_async_copy(ref, ref, sem).wait()


def kernel(
    tgt_in, nbr_in, cnt_in, pos_in, vel_in, smooth_in, mass_in, energy_in, slots_out, least_out,
    tgt, nbr, cnt, pos, vel, smooth, mass, energy, base_of,
    pool, mfpool, table, rows, cols, stash, coll, res, outsend, outbuf,
    mine, zbuf, xbuf, last, final,
    load, dsend, drecv, tsend, trecv, fsend, frecv, osend, orecv, msend, mrecv,
):
    a = lax.axis_index("dom")
    g = lax.axis_index("grp")
    n_dom = lax.axis_size("dom")
    z, y, c = a // 16, (a // 2) % 8, a % 2
    column = (y == 0) & (c == 0) & (g == 0)
    zeroth = column & (z == 0)
    stand_in = (a == 1) & (g == 0)
    root = (z < 2) & jnp.logical_not(zeroth)
    hands_on = z == 4
    low, high = a > 0, a < n_dom - 1

    def dom_of(zz, yy, cc):
        return (zz * NY + yy) * 2 + cc

    others = [lax.rem(g + d, NG) for d in (2, 1, 3)]
    moves = [(dy, dx, dc) for dy in (4, 3, 5, 2, 6, 1, 7, 0) for dx in (2, 1, 3, 0) for dc in (0, 1) if dy or dx or dc]

    def with_plane(do):
        for k, (dy, dx, dc) in enumerate(moves):
            dom, grp = dom_of(z, lax.rem(y + dy, NY), lax.rem(c + dc, 2)), lax.rem(g + dx, NG)
            pl.when((dom > 0) | (grp > 0))(functools.partial(do, k, at(dom, grp)))

    loads = [
        pltpu.make_async_copy(src, dst, load.at[k])
        for k, (src, dst) in enumerate((
            (cnt_in, cnt), (smooth_in, smooth), (energy_in, energy), (tgt_in, tgt),
            (pos_in, pos), (vel_in, vel), (mass_in, mass), (nbr_in, nbr),
        ))
    ]
    for copy in loads:
        copy.start()

    barrier = pltpu.get_barrier_semaphore()

    def greet(to):
        pl.semaphore_signal(barrier, inc=1, device_id=to, device_id_type=MESH)

    for o in others:
        greet(at(a, o))

    @pl.when(low)
    def _():
        greet(at(a - 1, g))

    @pl.when(high)
    def _():
        greet(at(a + 1, g))

    @pl.when(root)
    def _():
        def child(k, _):
            greet(at(dom_of(lax.rem(z + 1 + k, NZ), y, c), g))
            return 0

        lax.fori_loop(0, NZ - 1, child, 0)
        with_plane(lambda k, p: greet(p))

    @pl.when(stand_in)
    def _():
        def child(k, _):
            greet(at(dom_of(k, 0, 0), 0))
            return 0

        lax.fori_loop(0, NZ, child, 0)

    lane = lax.broadcasted_iota(jnp.int32, (NB, W), 1)
    sub = lax.broadcasted_iota(jnp.int32, (NB, W), 0)
    for copy in loads[:3]:
        copy.wait()
    count = jnp.zeros((NB, W), jnp.int32)
    for b in range(NB):
        count = jnp.where(sub == b, cnt[b], count)
    active = lane < count
    h = smooth[...]
    u = energy[...]
    steps = jnp.where(active, CFL * h / jnp.sqrt(GAMMA * (GAMMA - 1.0) * u), 1e30)
    mine[...] = jnp.min(steps, axis=0, keepdims=True)

    wait_for = 3 + jnp.where(low, 1, 0) + jnp.where(high, 1, 0) + jnp.where(root, jnp.where(z == 0, len(moves), len(moves) + 1), 2)
    pl.semaphore_wait(barrier, wait_for)

    def report(zr):
        to, row = dom_of(zr, y, c), z
        if zr == 0:
            to, row = jnp.where(column, 1, to), jnp.where(column, NZ + z, z)
        return remote(mine, zbuf.at[pl.ds(row, 1)], msend.at[zr], mrecv.at[0], at(to, g))

    reports = ((0, (z > 0) | zeroth), (1, z != 1))
    for zr, there in reports:
        pl.when(there)(lambda zr=zr: report(zr).start())

    @pl.when(root & jnp.logical_not(stand_in))
    def _():
        zbuf[NZ : 2 * NZ, :] = jnp.full((NZ, W), 1e30, jnp.float32)

    @pl.when(root & (z == 0))
    def _():
        xbuf[0:1, :] = jnp.full((1, W), 1e30, jnp.float32)

    for copy in loads[3:]:
        copy.wait()
    m = mass[...]

    own = (NG + g) * 4 * NB
    for comp in range(3):
        for b in range(NB):
            piece = pl.ds(b * W, W)
            rows[comp * NB + b : comp * NB + b + 1, :] = (
                pos[comp : comp + 1, piece] + DRIFT * vel[comp : comp + 1, piece]
            )
        pool[pl.ds(pl.multiple_of(own + comp * NB, NB), NB), :] = rows[comp * NB : comp * NB + NB, :]
    pool[pl.ds(pl.multiple_of(own + 3 * NB, NB), NB), :] = m
    pool[pl.ds(EMPTY * 4, 4 * NB), :] = jnp.zeros((4 * NB, W), jnp.float32)
    mfpool[pl.ds(EMPTY, NB), :] = jnp.zeros((NB, W), jnp.float32)
    res[pl.ds(4 * NB, NB), :] = jnp.zeros((NB, W), jnp.float32)

    targets = [tgt[b] for b in range(NB)]
    ranks = []
    for b in range(NB):
        r = jnp.int32(0)
        for e in range(b):
            r = r + jnp.where(targets[e] == targets[b], 1, 0)
        ranks.append(r)
    places = [targets[b] * CAP + ranks[b] for b in range(NB)]
    for s in range(NG * CAP):
        found = jnp.int32(NB)
        for b in range(NB):
            found = jnp.where(places[b] == s, b, found)
        table[NG + g, s] = found

    @pl.when(jnp.logical_not(low))
    def _():
        for d in range(NG):
            for s in range(NG * CAP):
                table[d, s] = jnp.int32(NB)

    @pl.when(jnp.logical_not(high))
    def _():
        for d in range(NG):
            for s in range(NG * CAP):
                table[2 * NG + d, s] = jnp.int32(NB)

    def piece_at(ref, per, i, d):
        return ref.at[pl.ds(pl.multiple_of((i * NG + lax.rem(g + d, NG)) * per, per), per)]

    def over_group(ref, per, send, recv, d):
        part = piece_at(ref, per, 1, 0)
        return remote(part, part, send.at[0], recv.at[NG - d - 1], at(a, lax.rem(g + d, NG)))

    def to_side(ref, per, send, recv, d, up):
        src, dst = piece_at(ref, per, 1, d), piece_at(ref, per, 0 if up else 2, d)
        k = 1 if up else 2
        return remote(src, dst, send.at[k], recv.at[k + 2], at(a + (1 if up else -1), g))

    def sides(parts, d, do):
        for up, there in ((True, high), (False, low)):
            @pl.when(there)
            def _():
                for part in parts:
                    do(to_side(*part, d, up))

    def gathered(parts, between):
        for d in (2, 1, 3):
            for part in parts:
                over_group(*part, d).start()
        sides(parts, 0, lambda copy: copy.start())
        between()
        for d in (1, 3, 2):
            for ref, per, send, recv in parts:
                landed(ref.at[pl.ds(0, per)], recv.at[d - 1])
            sides(parts, d, lambda copy: copy.start())
        for k, there in ((3, low), (4, high)):
            @pl.when(there)
            def _():
                for ref, per, send, recv in parts:
                    landed(ref.at[pl.ds(0, NG * per)], recv.at[k])

    def sent(parts):
        for k, pieces, there in ((0, 3, None), (1, NG, high), (2, NG, low)):
            def left():
                for ref, per, send, recv in parts:
                    landed(ref.at[pl.ds(0, pieces * per)], send.at[k])

            left() if there is None else pl.when(there)(left)

    first = ((pool, 4 * NB, dsend, drecv), (table, 1, tsend, trecv))

    def columns():
        rows[3 * NB : 4 * NB, :] = h * h

        def one(b, _):
            for comp in range(4):
                row = rows[pl.ds(comp * NB + b, 1), :]
                cols[comp, pl.ds(pl.multiple_of(b * W, W), W), :] = jnp.transpose(jnp.broadcast_to(row, (W, W)))
            return 0

        lax.fori_loop(0, NB, one, 0)

    gathered(first, columns)

    def partner(b, k):
        if k == 0:
            return NG + g, b
        n = nbr[k - 1, b]
        cell, s = n // 16, n % 16
        i, j = cell // 3, cell % 3
        t = tgt[b] + j - 1
        d = i * NG + s // CAP
        e = table[d, jnp.clip(t, 0, NG - 1) * CAP + s % CAP]
        there = (t >= 0) & (t < NG) & (a + i >= 1) & (a + i <= n_dom) & (e < NB)
        return jnp.where(there, d, 3 * NG), jnp.where(there, e, 0)

    def find(b):
        who = [partner(b, k) for k in range(5)]
        for k, (d, e) in enumerate(who):
            base_of[b * 5 + k] = d * NB + e
        return who

    lane_of = lax.broadcasted_iota(jnp.int32, (CH, W), 1)

    def keep(q, b, sums):
        here = slice(q * CH, (q + 1) * CH)
        kept = coll[here, :]
        for k, s in enumerate(sums):
            kept = jnp.where(lane_of == k * NB + b, jnp.sum(s, axis=1, keepdims=True), kept)
        coll[here, :] = kept

    def stashed(b, k, q):
        return pl.ds(pl.multiple_of((b * 5 + k) * W + q * CH, CH), CH)

    def density_pairs(b, _):
        who = find(b)
        for q in range(W // CH):
            mine_at = pl.ds(pl.multiple_of(b * W + q * CH, CH), CH)
            cx, cy, cz, ch2 = (cols[comp, mine_at, :] for comp in range(4))
            sums = [jnp.zeros((CH, W), jnp.float32) for _ in range(4)]
            for k, (d, e) in enumerate(who):
                base = d * (4 * NB) + e
                dx = cx - pool[pl.ds(base, 1), :]
                dy = cy - pool[pl.ds(base + NB, 1), :]
                dz = cz - pool[pl.ds(base + 2 * NB, 1), :]
                w = jnp.maximum(ch2 - (dx * dx + dy * dy + dz * dz), 0.0)
                w2 = w * w
                m_j = pool[pl.ds(base + 3 * NB, 1), :]
                parts = []
                for comp, delta in enumerate((dx, dy, dz)):
                    part = w2 * delta
                    stash[comp, stashed(b, k, q), :] = part
                    parts.append(m_j * part)
                parts.append(m_j * (w2 * w))
                sums = [s + p for s, p in zip(sums, parts)]
            keep(q, b, sums)
        return 0

    def force_pairs(b, _):
        who = [base_of[b * 5 + k] for k in range(5)]
        for q in range(W // CH):
            sums = [jnp.zeros((CH, W), jnp.float32) for _ in range(3)]
            for k, base in enumerate(who):
                mf_j = mfpool[pl.ds(base, 1), :]
                sums = [s + mf_j * stash[comp, stashed(b, k, q), :] for comp, s in enumerate(sums)]
            keep(q, b, sums)
        return 0

    def pairs(block):
        coll[...] = jnp.zeros((W, W), jnp.float32)
        def two(b, _):
            for k in range(4):
                block(4 * b + k, 0)
            return 0

        lax.fori_loop(0, NB // 4, two, 0)
        return jnp.transpose(coll[...])

    inv_h = 1.0 / h
    ih3 = inv_h * inv_h * inv_h
    ih9 = KNORM * (ih3 * ih3 * ih3)

    found = pairs(density_pairs)
    rho = ih9 * found[3 * NB : 4 * NB, :]
    factor = (GAMMA - 1.0) * u / rho
    mfpool[pl.ds(pl.multiple_of((NG + g) * NB, NB), NB), :] = m * factor
    res[0:NB, :] = rho
    for comp in range(3):
        res[(1 + comp) * NB : (2 + comp) * NB, :] = factor * found[comp * NB : (comp + 1) * NB, :]

    part = mfpool.at[pl.ds(pl.multiple_of((NG + g) * NB, NB), NB)]

    def factors(i):
        dst = mfpool.at[pl.ds(pl.multiple_of(((1 - i) * NG + g) * NB, NB), NB)]
        to = others if i == 0 else others + [g]
        return [
            remote(part, dst, fsend.at[i + 1], frecv.at[1 - i], at(a + i, o)) for k, o in enumerate(to)
        ]

    def on_sides(do):
        for i, there in ((1, high), (-1, low)):
            pl.when(there)(functools.partial(do, i))

    def start_factors(i):
        for copy in factors(i):
            copy.start()

    def sent_factors(i):
        landed(mfpool.at[pl.ds(0, (3 if i == 0 else NG) * NB)], fsend.at[i + 1])

    on_sides(start_factors)
    start_factors(0)
    landed(mfpool.at[pl.ds(0, 3 * NB)], frecv.at[1])
    on_sides(lambda i: landed(mfpool.at[pl.ds(0, NG * NB)], frecv.at[1 + i]))

    found = pairs(force_pairs)
    for comp in range(3):
        here = slice((1 + comp) * NB, (2 + comp) * NB)
        total = 6.0 * ih9 * (res[here, :] + found[comp * NB : (comp + 1) * NB, :])
        res[here, :] = jnp.where(active, total, 0.0)

    @pl.when(root)
    def _():
        zbuf[pl.ds(z, 1), :] = mine[...]

        @pl.when(stand_in)
        def _():
            landed(zbuf.at[pl.ds(0, 2 * NZ - 1)], mrecv.at[0])

        @pl.when(jnp.logical_not(stand_in))
        def _():
            landed(zbuf.at[pl.ds(0, NZ - 1)], mrecv.at[0])

        least = jnp.min(zbuf[...], axis=0, keepdims=True)
        index = (y * 2 + c) * NG + g
        last[...] = least
        xbuf[pl.ds(index, 1), :] = least
        with_plane(lambda k, p: remote(last, xbuf.at[pl.ds(index, 1)], msend.at[2], mrecv.at[1], p).start())

    for t in range(NG):
        for r in range(CAP):
            e = table[NG + g, t * CAP + r]
            for comp in range(4):
                source = jnp.where(e < NB, comp * NB + e, 4 * NB)
                outsend[t, comp * CAP + r : comp * CAP + r + 1, :] = res[pl.ds(source, 1), :]
    results = [remote(outsend.at[o], outbuf.at[g], osend, orecv, at(a, o)) for o in others]
    for copy in results:
        copy.start()
    outbuf[g] = outsend[g]

    landed(outbuf.at[pl.ds(0, 3)], orecv)
    slots_out[...] = outbuf[...]

    @pl.when(root)
    def _():
        @pl.when(z == 0)
        def _():
            landed(xbuf.at[pl.ds(0, len(moves) - 1)], mrecv.at[1])

        @pl.when(z != 0)
        def _():
            landed(xbuf.at[pl.ds(0, len(moves))], mrecv.at[1])

        final[...] = jnp.min(xbuf[...], axis=0, keepdims=True)

    def give(k, to):
        return remote(final, final, msend.at[k], mrecv.at[2], at(dom_of(to, y, c), g))

    @pl.when(z == 1)
    def _():
        for to in (4, 3, 2):
            give(3, to).start()
        pl.when(column)(lambda: give(4, 0).start())

    @pl.when(jnp.logical_not(root))
    def _():
        landed(final, mrecv.at[2])

    @pl.when(hands_on)
    def _():
        for to in range(NZ - 1, 4, -1):
            give(3, to).start()

    least_out[...] = final[...]

    sent(first)
    sent_factors(0)
    on_sides(sent_factors)
    landed(outbuf.at[pl.ds(0, 3)], osend)
    for zr, there in reports:
        pl.when(there)(lambda zr=zr: report(zr).wait_send())

    @pl.when(root)
    def _():
        @pl.when(z == 0)
        def _():
            landed(xbuf.at[pl.ds(0, len(moves) - 1)], msend.at[2])

        @pl.when(z != 0)
        def _():
            landed(xbuf.at[pl.ds(0, len(moves))], msend.at[2])

    @pl.when(z == 1)
    def _():
        landed(xbuf.at[pl.ds(0, 3)], msend.at[3])
        pl.when(column)(lambda: landed(final, msend.at[4]))

    @pl.when(hands_on)
    def _():
        landed(xbuf.at[pl.ds(0, NZ - 5)], msend.at[3])


def unpack(slots_in, least_in, dens_out, acc_out, ts_out):
    for s in range(NG):
        dens_out[s * CAP : (s + 1) * CAP, :] = slots_in[s, 0:CAP, :]
        for comp in range(3):
            for r in range(CAP):
                row = (1 + comp) * CAP + r
                slot = s * CAP + r
                acc_out[comp : comp + 1, slot * W : (slot + 1) * W] = slots_in[s, row : row + 1, :]
    ts_out[0] = jnp.min(least_in[...])


def body(positions, velocity, smoothing, mass, energy, targets, neighbours, counts):
    f32 = jnp.float32
    slots = NG * CAP
    vmem, smem = pl.BlockSpec(memory_space=pltpu.VMEM), pl.BlockSpec(memory_space=pltpu.SMEM)
    sem = pltpu.SemaphoreType.DMA
    packed, least = pl.pallas_call(
        kernel,
        out_shape=(pltpu.VMEM((NG, 4 * CAP, W), f32), pltpu.VMEM((1, W), f32)),
        in_specs=[pl.BlockSpec(memory_space=pl.ANY)] * 8,
        out_specs=(vmem, vmem),
        scratch_shapes=[
            pltpu.SMEM((NB,), jnp.int32),
            pltpu.SMEM((4, NB), jnp.int32),
            pltpu.SMEM((NB,), jnp.int32),
            pltpu.VMEM((3, NB * W), f32),
            pltpu.VMEM((3, NB * W), f32),
            pltpu.VMEM((NB, W), f32),
            pltpu.VMEM((NB, W), f32),
            pltpu.VMEM((NB, W), f32),
            pltpu.SMEM((5 * NB,), jnp.int32),
            pltpu.VMEM(((EMPTY + NB) * 4, W), f32),
            pltpu.VMEM((EMPTY + NB, W), f32),
            pltpu.SMEM((3 * NG, 16), jnp.int32),
            pltpu.VMEM((4 * NB, W), f32),
            pltpu.VMEM((4, NB * W, W), f32),
            pltpu.VMEM((3, 5 * NB * W, W), f32),
            pltpu.VMEM((W, W), f32),
            pltpu.VMEM((5 * NB, W), f32),
            pltpu.VMEM((NG, 4 * CAP, W), f32),
            pltpu.VMEM((NG, 4 * CAP, W), f32),
            pltpu.VMEM((1, W), f32),
            pltpu.VMEM((2 * NZ, W), f32),
            pltpu.VMEM((2 * NY * NG, W), f32),
            pltpu.VMEM((1, W), f32),
            pltpu.VMEM((1, W), f32),
            sem((8,)), sem((3,)), sem((5,)), sem((3,)), sem((5,)), sem((3,)), sem((3,)),
            sem, sem, sem((5,)), sem((3,)),
        ],
        compiler_params=pltpu.CompilerParams(collective_id=0, has_side_effects=True),
    )(
        targets.reshape(-1), neighbours.T, counts, positions, velocity,
        smoothing.reshape(NB, W), mass.reshape(NB, W), energy.reshape(NB, W),
    )
    dens, acc, ts = pl.pallas_call(
        unpack,
        out_shape=(
            jax.ShapeDtypeStruct((slots, W), f32),
            jax.ShapeDtypeStruct((3, slots * W), f32),
            jax.ShapeDtypeStruct((1,), f32),
        ),
        in_specs=[vmem] * 2,
        out_specs=(vmem, vmem, smem),
    )(*(pltpu.with_memory_space_constraint(v, pltpu.VMEM) for v in (packed, least)))
    return dens.reshape(-1), acc, ts


def solution(mesh):
    both = ("dom", "grp")
    return jax.shard_map(
        body,
        mesh=mesh,
        in_specs=(P(None, both), P(None, both), P(both), P(both), P(both), P(both, None), P(both, None), P(both)),
        out_specs=(P(both), P(None, both), P()),
        check_vma=False,
    )
```

```python
import functools
import math

import jax
import jax.numpy as jnp
from jax import lax
from jax.experimental import pallas as pl
from jax.experimental.pallas import tpu as pltpu
from jax.sharding import PartitionSpec as P

MESH = pl.DeviceIdType.MESH
CAP = 4
DRIFT = 0.05
GAMMA = 5.0 / 3.0
CFL = 0.3
KNORM = 315.0 / (64.0 * math.pi)

NB = 8
NG = 4
NZ, NY = 16, 8
W = 128
EMPTY = 12 * NB
CH = 32


def at(dom, grp):
    return {"dom": dom, "grp": grp}


def remote(src, dst, send, recv, to):
    return pltpu.make_async_remote_copy(
        src_ref=src, dst_ref=dst, send_sem=send, recv_sem=recv, device_id=to, device_id_type=MESH
    )


def landed(ref, sem):
    pltpu.make_async_copy(ref, ref, sem).wait()


def kernel(
    tgt_in, nbr_in, cnt_in, pos_in, vel_in, smooth_in, mass_in, energy_in, slots_out, least_out,
    tgt, nbr, cnt, pos, vel, smooth, mass, energy, base_of,
    pool, mfpool, table, rows, cols, stash, coll, res, outsend, outbuf,
    mine, zbuf, xbuf, last, final,
    load, dsend, drecv, tsend, trecv, fsend, frecv, osend, orecv, msend, mrecv,
):
    a = lax.axis_index("dom")
    g = lax.axis_index("grp")
    n_dom = lax.axis_size("dom")
    z, y, c = a // 16, (a // 2) % 8, a % 2
    column = (y == 0) & (c == 0) & (g == 0)
    zeroth = column & (z == 0)
    stand_in = (a == 1) & (g == 0)
    root = (z < 2) & jnp.logical_not(zeroth)
    hands_on = z == 4
    low, high = a > 0, a < n_dom - 1

    def dom_of(zz, yy, cc):
        return (zz * NY + yy) * 2 + cc

    others = [lax.rem(g + d, NG) for d in (2, 1, 3)]
    moves = [(dy, dx, dc) for dy in (4, 3, 5, 2, 6, 1, 7, 0) for dx in (2, 1, 3, 0) for dc in (0, 1) if dy or dx or dc]

    def with_plane(do):
        for k, (dy, dx, dc) in enumerate(moves):
            dom, grp = dom_of(z, lax.rem(y + dy, NY), lax.rem(c + dc, 2)), lax.rem(g + dx, NG)
            pl.when((dom > 0) | (grp > 0))(functools.partial(do, k, at(dom, grp)))

    loads = [
        pltpu.make_async_copy(src, dst, load.at[k])
        for k, (src, dst) in enumerate((
            (cnt_in, cnt), (smooth_in, smooth), (energy_in, energy), (tgt_in, tgt),
            (pos_in, pos), (vel_in, vel), (mass_in, mass), (nbr_in, nbr),
        ))
    ]
    for copy in loads:
        copy.start()

    barrier = pltpu.get_barrier_semaphore()

    def greet(to):
        pl.semaphore_signal(barrier, inc=1, device_id=to, device_id_type=MESH)

    for o in others:
        greet(at(a, o))

    @pl.when(low)
    def _():
        greet(at(a - 1, g))

    @pl.when(high)
    def _():
        greet(at(a + 1, g))

    @pl.when(root)
    def _():
        def child(k, _):
            greet(at(dom_of(lax.rem(z + 1 + k, NZ), y, c), g))
            return 0

        lax.fori_loop(0, NZ - 1, child, 0)
        with_plane(lambda k, p: greet(p))

    @pl.when(stand_in)
    def _():
        def child(k, _):
            greet(at(dom_of(k, 0, 0), 0))
            return 0

        lax.fori_loop(0, NZ, child, 0)

    lane = lax.broadcasted_iota(jnp.int32, (NB, W), 1)
    sub = lax.broadcasted_iota(jnp.int32, (NB, W), 0)
    for copy in loads[:3]:
        copy.wait()
    count = jnp.zeros((NB, W), jnp.int32)
    for b in range(NB):
        count = jnp.where(sub == b, cnt[b], count)
    active = lane < count
    h = smooth[...]
    u = energy[...]
    steps = jnp.where(active, CFL * h / jnp.sqrt(GAMMA * (GAMMA - 1.0) * u), 1e30)
    mine[...] = jnp.min(steps, axis=0, keepdims=True)

    wait_for = 3 + jnp.where(low, 1, 0) + jnp.where(high, 1, 0) + jnp.where(root, jnp.where(z == 0, len(moves), len(moves) + 1), 2)
    pl.semaphore_wait(barrier, wait_for)

    def report(zr):
        to, row = dom_of(zr, y, c), z
        if zr == 0:
            to, row = jnp.where(column, 1, to), jnp.where(column, NZ + z, z)
        return remote(mine, zbuf.at[pl.ds(row, 1)], msend.at[zr], mrecv.at[0], at(to, g))

    reports = ((0, (z > 0) | zeroth), (1, z != 1))
    for zr, there in reports:
        pl.when(there)(lambda zr=zr: report(zr).start())

    @pl.when(root & jnp.logical_not(stand_in))
    def _():
        zbuf[NZ : 2 * NZ, :] = jnp.full((NZ, W), 1e30, jnp.float32)

    @pl.when(root & (z == 0))
    def _():
        xbuf[0:1, :] = jnp.full((1, W), 1e30, jnp.float32)

    for copy in loads[3:]:
        copy.wait()
    m = mass[...]

    own = (NG + g) * 4 * NB
    for comp in range(3):
        for b in range(NB):
            piece = pl.ds(b * W, W)
            rows[comp * NB + b : comp * NB + b + 1, :] = (
                pos[comp : comp + 1, piece] + DRIFT * vel[comp : comp + 1, piece]
            )
        pool[pl.ds(pl.multiple_of(own + comp * NB, NB), NB), :] = rows[comp * NB : comp * NB + NB, :]
    pool[pl.ds(pl.multiple_of(own + 3 * NB, NB), NB), :] = m
    pool[pl.ds(EMPTY * 4, 4 * NB), :] = jnp.zeros((4 * NB, W), jnp.float32)
    mfpool[pl.ds(EMPTY, NB), :] = jnp.zeros((NB, W), jnp.float32)
    res[pl.ds(4 * NB, NB), :] = jnp.zeros((NB, W), jnp.float32)

    targets = [tgt[b] for b in range(NB)]
    ranks = []
    for b in range(NB):
        r = jnp.int32(0)
        for e in range(b):
            r = r + jnp.where(targets[e] == targets[b], 1, 0)
        ranks.append(r)
    places = [targets[b] * CAP + ranks[b] for b in range(NB)]
    for s in range(NG * CAP):
        found = jnp.int32(NB)
        for b in range(NB):
            found = jnp.where(places[b] == s, b, found)
        table[NG + g, s] = found

    @pl.when(jnp.logical_not(low))
    def _():
        for d in range(NG):
            for s in range(NG * CAP):
                table[d, s] = jnp.int32(NB)

    @pl.when(jnp.logical_not(high))
    def _():
        for d in range(NG):
            for s in range(NG * CAP):
                table[2 * NG + d, s] = jnp.int32(NB)

    def piece_at(ref, per, i, d):
        return ref.at[pl.ds(pl.multiple_of((i * NG + lax.rem(g + d, NG)) * per, per), per)]

    def over_group(ref, per, send, recv, d):
        part = piece_at(ref, per, 1, 0)
        return remote(part, part, send.at[0], recv.at[NG - d - 1], at(a, lax.rem(g + d, NG)))

    def to_side(ref, per, send, recv, d, up):
        src, dst = piece_at(ref, per, 1, d), piece_at(ref, per, 0 if up else 2, d)
        k = 1 if up else 2
        return remote(src, dst, send.at[k], recv.at[k + 2], at(a + (1 if up else -1), g))

    def sides(parts, d, do):
        for up, there in ((True, high), (False, low)):
            @pl.when(there)
            def _():
                for part in parts:
                    do(to_side(*part, d, up))

    def gathered(parts, between):
        for d in (2, 1, 3):
            for part in parts:
                over_group(*part, d).start()
        sides(parts, 0, lambda copy: copy.start())
        between()
        for d in (1, 3, 2):
            for ref, per, send, recv in parts:
                landed(ref.at[pl.ds(0, per)], recv.at[d - 1])
            sides(parts, d, lambda copy: copy.start())
        for k, there in ((3, low), (4, high)):
            @pl.when(there)
            def _():
                for ref, per, send, recv in parts:
                    landed(ref.at[pl.ds(0, NG * per)], recv.at[k])

    def sent(parts):
        for k, pieces, there in ((0, 3, None), (1, NG, high), (2, NG, low)):
            def left():
                for ref, per, send, recv in parts:
                    landed(ref.at[pl.ds(0, pieces * per)], send.at[k])

            left() if there is None else pl.when(there)(left)

    first = ((pool, 4 * NB, dsend, drecv), (table, 1, tsend, trecv))

    def columns():
        rows[3 * NB : 4 * NB, :] = h * h

        def one(b, _):
            for comp in range(4):
                row = rows[pl.ds(comp * NB + b, 1), :]
                cols[comp, pl.ds(pl.multiple_of(b * W, W), W), :] = jnp.transpose(jnp.broadcast_to(row, (W, W)))
            return 0

        lax.fori_loop(0, NB, one, 0)

    gathered(first, columns)

    def partner(b, k):
        if k == 0:
            return NG + g, b
        n = nbr[k - 1, b]
        cell, s = n // 16, n % 16
        i, j = cell // 3, cell % 3
        t = tgt[b] + j - 1
        d = i * NG + s // CAP
        e = table[d, jnp.clip(t, 0, NG - 1) * CAP + s % CAP]
        there = (t >= 0) & (t < NG) & (a + i >= 1) & (a + i <= n_dom) & (e < NB)
        return jnp.where(there, d, 3 * NG), jnp.where(there, e, 0)

    def find(b):
        who = [partner(b, k) for k in range(5)]
        for k, (d, e) in enumerate(who):
            base_of[b * 5 + k] = d * NB + e
        return who

    lane_of = lax.broadcasted_iota(jnp.int32, (CH, W), 1)

    def keep(q, b, sums):
        here = slice(q * CH, (q + 1) * CH)
        kept = coll[here, :]
        for k, s in enumerate(sums):
            kept = jnp.where(lane_of == k * NB + b, jnp.sum(s, axis=1, keepdims=True), kept)
        coll[here, :] = kept

    def stashed(b, k, q):
        return pl.ds(pl.multiple_of((b * 5 + k) * W + q * CH, CH), CH)

    def density_pairs(b, _):
        who = find(b)
        for q in range(W // CH):
            mine_at = pl.ds(pl.multiple_of(b * W + q * CH, CH), CH)
            cx, cy, cz, ch2 = (cols[comp, mine_at, :] for comp in range(4))
            sums = [jnp.zeros((CH, W), jnp.float32) for _ in range(4)]
            for k, (d, e) in enumerate(who):
                base = d * (4 * NB) + e
                dx = cx - pool[pl.ds(base, 1), :]
                dy = cy - pool[pl.ds(base + NB, 1), :]
                dz = cz - pool[pl.ds(base + 2 * NB, 1), :]
                w = jnp.maximum(ch2 - (dx * dx + dy * dy + dz * dz), 0.0)
                w2 = w * w
                m_j = pool[pl.ds(base + 3 * NB, 1), :]
                parts = []
                for comp, delta in enumerate((dx, dy, dz)):
                    part = w2 * delta
                    stash[comp, stashed(b, k, q), :] = part
                    parts.append(m_j * part)
                parts.append(m_j * (w2 * w))
                sums = [s + p for s, p in zip(sums, parts)]
            keep(q, b, sums)
        return 0

    def force_pairs(b, _):
        who = [base_of[b * 5 + k] for k in range(5)]
        for q in range(W // CH):
            sums = [jnp.zeros((CH, W), jnp.float32) for _ in range(3)]
            for k, base in enumerate(who):
                mf_j = mfpool[pl.ds(base, 1), :]
                sums = [s + mf_j * stash[comp, stashed(b, k, q), :] for comp, s in enumerate(sums)]
            keep(q, b, sums)
        return 0

    def pairs(block):
        coll[...] = jnp.zeros((W, W), jnp.float32)
        def two(b, _):
            for k in range(4):
                block(4 * b + k, 0)
            return 0

        lax.fori_loop(0, NB // 4, two, 0)
        return jnp.transpose(coll[...])

    inv_h = 1.0 / h
    ih3 = inv_h * inv_h * inv_h
    ih9 = KNORM * (ih3 * ih3 * ih3)

    found = pairs(density_pairs)
    rho = ih9 * found[3 * NB : 4 * NB, :]
    factor = (GAMMA - 1.0) * u / rho
    mfpool[pl.ds(pl.multiple_of((NG + g) * NB, NB), NB), :] = m * factor
    res[0:NB, :] = rho
    for comp in range(3):
        res[(1 + comp) * NB : (2 + comp) * NB, :] = factor * found[comp * NB : (comp + 1) * NB, :]

    part = mfpool.at[pl.ds(pl.multiple_of((NG + g) * NB, NB), NB)]

    def factors(i):
        dst = mfpool.at[pl.ds(pl.multiple_of(((1 - i) * NG + g) * NB, NB), NB)]
        to = others if i == 0 else others + [g]
        return [
            remote(part, dst, fsend.at[i + 1], frecv.at[1 - i], at(a + i, o)) for k, o in enumerate(to)
        ]

    def on_sides(do):
        for i, there in ((1, high), (-1, low)):
            pl.when(there)(functools.partial(do, i))

    def start_factors(i):
        for copy in factors(i):
            copy.start()

    def sent_factors(i):
        landed(mfpool.at[pl.ds(0, (3 if i == 0 else NG) * NB)], fsend.at[i + 1])

    on_sides(start_factors)
    start_factors(0)
    landed(mfpool.at[pl.ds(0, 3 * NB)], frecv.at[1])
    on_sides(lambda i: landed(mfpool.at[pl.ds(0, NG * NB)], frecv.at[1 + i]))

    found = pairs(force_pairs)
    for comp in range(3):
        here = slice((1 + comp) * NB, (2 + comp) * NB)
        total = 6.0 * ih9 * (res[here, :] + found[comp * NB : (comp + 1) * NB, :])
        res[here, :] = jnp.where(active, total, 0.0)

    @pl.when(root)
    def _():
        zbuf[pl.ds(z, 1), :] = mine[...]

        @pl.when(stand_in)
        def _():
            landed(zbuf.at[pl.ds(0, 2 * NZ - 1)], mrecv.at[0])

        @pl.when(jnp.logical_not(stand_in))
        def _():
            landed(zbuf.at[pl.ds(0, NZ - 1)], mrecv.at[0])

        least = jnp.min(zbuf[...], axis=0, keepdims=True)
        index = (y * 2 + c) * NG + g
        last[...] = least
        xbuf[pl.ds(index, 1), :] = least
        with_plane(lambda k, p: remote(last, xbuf.at[pl.ds(index, 1)], msend.at[2], mrecv.at[1], p).start())

    for t in range(NG):
        for r in range(CAP):
            e = table[NG + g, t * CAP + r]
            for comp in range(4):
                source = jnp.where(e < NB, comp * NB + e, 4 * NB)
                outsend[t, comp * CAP + r : comp * CAP + r + 1, :] = res[pl.ds(source, 1), :]
    results = [remote(outsend.at[o], outbuf.at[g], osend, orecv, at(a, o)) for o in others]
    for copy in results:
        copy.start()
    outbuf[g] = outsend[g]

    landed(outbuf.at[pl.ds(0, 3)], orecv)
    slots_out[...] = outbuf[...]

    sent(first)
    sent_factors(0)
    on_sides(sent_factors)
    landed(outbuf.at[pl.ds(0, 3)], osend)
    for zr, there in reports:
        pl.when(there)(lambda zr=zr: report(zr).wait_send())

    @pl.when(root)
    def _():
        @pl.when(z == 0)
        def _():
            landed(xbuf.at[pl.ds(0, len(moves) - 1)], msend.at[2])

        @pl.when(z != 0)
        def _():
            landed(xbuf.at[pl.ds(0, len(moves))], msend.at[2])

    @pl.when(root)
    def _():
        @pl.when(z == 0)
        def _():
            landed(xbuf.at[pl.ds(0, len(moves) - 1)], mrecv.at[1])

        @pl.when(z != 0)
        def _():
            landed(xbuf.at[pl.ds(0, len(moves))], mrecv.at[1])

        final[...] = jnp.min(xbuf[...], axis=0, keepdims=True)

    def give(k, to):
        return remote(final, final, msend.at[k], mrecv.at[2], at(dom_of(to, y, c), g))

    @pl.when(z == 1)
    def _():
        for to in (4, 3, 2):
            give(3, to).start()
        pl.when(column)(lambda: give(4, 0).start())

    @pl.when(jnp.logical_not(root))
    def _():
        landed(final, mrecv.at[2])

    @pl.when(hands_on)
    def _():
        for to in range(NZ - 1, 4, -1):
            give(3, to).start()

    least_out[...] = final[...]

    @pl.when(z == 1)
    def _():
        landed(xbuf.at[pl.ds(0, 3)], msend.at[3])
        pl.when(column)(lambda: landed(final, msend.at[4]))

    @pl.when(hands_on)
    def _():
        landed(xbuf.at[pl.ds(0, NZ - 5)], msend.at[3])


def unpack(slots_in, least_in, dens_out, acc_out, ts_out):
    for s in range(NG):
        dens_out[s * CAP : (s + 1) * CAP, :] = slots_in[s, 0:CAP, :]
        for comp in range(3):
            for r in range(CAP):
                row = (1 + comp) * CAP + r
                slot = s * CAP + r
                acc_out[comp : comp + 1, slot * W : (slot + 1) * W] = slots_in[s, row : row + 1, :]
    ts_out[0] = jnp.min(least_in[...])


def body(positions, velocity, smoothing, mass, energy, targets, neighbours, counts):
    f32 = jnp.float32
    slots = NG * CAP
    vmem, smem = pl.BlockSpec(memory_space=pltpu.VMEM), pl.BlockSpec(memory_space=pltpu.SMEM)
    sem = pltpu.SemaphoreType.DMA
    packed, least = pl.pallas_call(
        kernel,
        out_shape=(pltpu.VMEM((NG, 4 * CAP, W), f32), pltpu.VMEM((1, W), f32)),
        in_specs=[pl.BlockSpec(memory_space=pl.ANY)] * 8,
        out_specs=(vmem, vmem),
        scratch_shapes=[
            pltpu.SMEM((NB,), jnp.int32),
            pltpu.SMEM((4, NB), jnp.int32),
            pltpu.SMEM((NB,), jnp.int32),
            pltpu.VMEM((3, NB * W), f32),
            pltpu.VMEM((3, NB * W), f32),
            pltpu.VMEM((NB, W), f32),
            pltpu.VMEM((NB, W), f32),
            pltpu.VMEM((NB, W), f32),
            pltpu.SMEM((5 * NB,), jnp.int32),
            pltpu.VMEM(((EMPTY + NB) * 4, W), f32),
            pltpu.VMEM((EMPTY + NB, W), f32),
            pltpu.SMEM((3 * NG, 16), jnp.int32),
            pltpu.VMEM((4 * NB, W), f32),
            pltpu.VMEM((4, NB * W, W), f32),
            pltpu.VMEM((3, 5 * NB * W, W), f32),
            pltpu.VMEM((W, W), f32),
            pltpu.VMEM((5 * NB, W), f32),
            pltpu.VMEM((NG, 4 * CAP, W), f32),
            pltpu.VMEM((NG, 4 * CAP, W), f32),
            pltpu.VMEM((1, W), f32),
            pltpu.VMEM((2 * NZ, W), f32),
            pltpu.VMEM((2 * NY * NG, W), f32),
            pltpu.VMEM((1, W), f32),
            pltpu.VMEM((1, W), f32),
            sem((8,)), sem((3,)), sem((5,)), sem((3,)), sem((5,)), sem((3,)), sem((3,)),
            sem, sem, sem((5,)), sem((3,)),
        ],
        compiler_params=pltpu.CompilerParams(collective_id=0, has_side_effects=True),
    )(
        targets.reshape(-1), neighbours.T, counts, positions, velocity,
        smoothing.reshape(NB, W), mass.reshape(NB, W), energy.reshape(NB, W),
    )
    dens, acc, ts = pl.pallas_call(
        unpack,
        out_shape=(
            jax.ShapeDtypeStruct((slots, W), f32),
            jax.ShapeDtypeStruct((3, slots * W), f32),
            jax.ShapeDtypeStruct((1,), f32),
        ),
        in_specs=[vmem] * 2,
        out_specs=(vmem, vmem, smem),
    )(*(pltpu.with_memory_space_constraint(v, pltpu.VMEM) for v in (packed, least)))
    return dens.reshape(-1), acc, ts


def solution(mesh):
    both = ("dom", "grp")
    return jax.shard_map(
        body,
        mesh=mesh,
        in_specs=(P(None, both), P(None, both), P(both), P(both), P(both), P(both, None), P(both, None), P(both)),
        out_specs=(P(both), P(None, both), P()),
        check_vma=False,
    )
```

```python
import functools
import math

import jax
import jax.numpy as jnp
from jax import lax
from jax.experimental import pallas as pl
from jax.experimental.pallas import tpu as pltpu
from jax.sharding import PartitionSpec as P

MESH = pl.DeviceIdType.MESH
CAP = 4
DRIFT = 0.05
GAMMA = 5.0 / 3.0
CFL = 0.3
KNORM = 315.0 / (64.0 * math.pi)

NB = 8
NG = 4
NZ, NY = 16, 8
W = 128
EMPTY = 12 * NB
CH = 32


def at(dom, grp):
    return {"dom": dom, "grp": grp}


def remote(src, dst, send, recv, to):
    return pltpu.make_async_remote_copy(
        src_ref=src, dst_ref=dst, send_sem=send, recv_sem=recv, device_id=to, device_id_type=MESH
    )


def landed(ref, sem):
    pltpu.make_async_copy(ref, ref, sem).wait()


def kernel(
    tgt_in, nbr_in, cnt_in, pos_in, vel_in, smooth_in, mass_in, energy_in, slots_out, least_out,
    tgt, nbr, cnt, pos, vel, smooth, mass, energy, base_of,
    pool, mfpool, table, rows, cols, stash, coll, res, outsend, outbuf,
    mine, zbuf, xbuf, last, final,
    load, drecv, trecv, frecv, orecv, mrecv,
):
    a = lax.axis_index("dom")
    g = lax.axis_index("grp")
    n_dom = lax.axis_size("dom")
    z, y, c = a // 16, (a // 2) % 8, a % 2
    column = (y == 0) & (c == 0) & (g == 0)
    zeroth = column & (z == 0)
    stand_in = (a == 1) & (g == 0)
    root = (z < 2) & jnp.logical_not(zeroth)
    hands_on = z == 4
    low, high = a > 0, a < n_dom - 1

    def dom_of(zz, yy, cc):
        return (zz * NY + yy) * 2 + cc

    others = [lax.rem(g + d, NG) for d in (2, 1, 3)]
    moves = [(dy, dx, dc) for dy in (4, 3, 5, 2, 6, 1, 7, 0) for dx in (2, 1, 3, 0) for dc in (0, 1) if dy or dx or dc]

    def with_plane(do):
        for k, (dy, dx, dc) in enumerate(moves):
            dom, grp = dom_of(z, lax.rem(y + dy, NY), lax.rem(c + dc, 2)), lax.rem(g + dx, NG)
            pl.when((dom > 0) | (grp > 0))(functools.partial(do, k, at(dom, grp)))

    loads = [
        pltpu.make_async_copy(src, dst, load.at[k])
        for k, (src, dst) in enumerate((
            (cnt_in, cnt), (smooth_in, smooth), (energy_in, energy), (tgt_in, tgt),
            (pos_in, pos), (vel_in, vel), (mass_in, mass), (nbr_in, nbr),
        ))
    ]
    for copy in loads:
        copy.start()

    barrier = pltpu.get_barrier_semaphore()

    def greet(to):
        pl.semaphore_signal(barrier, inc=1, device_id=to, device_id_type=MESH)

    for o in others:
        greet(at(a, o))

    @pl.when(low)
    def _():
        greet(at(a - 1, g))

    @pl.when(high)
    def _():
        greet(at(a + 1, g))

    @pl.when(root)
    def _():
        def child(k, _):
            greet(at(dom_of(lax.rem(z + 1 + k, NZ), y, c), g))
            return 0

        lax.fori_loop(0, NZ - 1, child, 0)
        with_plane(lambda k, p: greet(p))

    @pl.when(stand_in)
    def _():
        def child(k, _):
            greet(at(dom_of(k, 0, 0), 0))
            return 0

        lax.fori_loop(0, NZ, child, 0)

    lane = lax.broadcasted_iota(jnp.int32, (NB, W), 1)
    sub = lax.broadcasted_iota(jnp.int32, (NB, W), 0)
    for copy in loads[:3]:
        copy.wait()
    count = jnp.zeros((NB, W), jnp.int32)
    for b in range(NB):
        count = jnp.where(sub == b, cnt[b], count)
    active = lane < count
    h = smooth[...]
    u = energy[...]
    steps = jnp.where(active, CFL * h / jnp.sqrt(GAMMA * (GAMMA - 1.0) * u), 1e30)
    mine[...] = jnp.min(steps, axis=0, keepdims=True)

    wait_for = 3 + jnp.where(low, 1, 0) + jnp.where(high, 1, 0) + jnp.where(root, jnp.where(z == 0, len(moves), len(moves) + 1), 2)
    pl.semaphore_wait(barrier, wait_for)

    def report(zr):
        to, row = dom_of(zr, y, c), z
        if zr == 0:
            to, row = jnp.where(column, 1, to), jnp.where(column, NZ + z, z)
        return remote(mine, zbuf.at[pl.ds(row, 1)], load.at[zr], mrecv.at[0], at(to, g))

    reports = ((0, (z > 0) | zeroth), (1, z != 1))
    for zr, there in reports:
        pl.when(there)(lambda zr=zr: report(zr).start())

    @pl.when(root & jnp.logical_not(stand_in))
    def _():
        zbuf[NZ : 2 * NZ, :] = jnp.full((NZ, W), 1e30, jnp.float32)

    @pl.when(root & (z == 0))
    def _():
        xbuf[0:1, :] = jnp.full((1, W), 1e30, jnp.float32)

    for copy in loads[3:]:
        copy.wait()
    m = mass[...]

    own = (NG + g) * 4 * NB
    for comp in range(3):
        for b in range(NB):
            piece = pl.ds(b * W, W)
            rows[comp * NB + b : comp * NB + b + 1, :] = (
                pos[comp : comp + 1, piece] + DRIFT * vel[comp : comp + 1, piece]
            )
        pool[pl.ds(pl.multiple_of(own + comp * NB, NB), NB), :] = rows[comp * NB : comp * NB + NB, :]
    pool[pl.ds(pl.multiple_of(own + 3 * NB, NB), NB), :] = m
    pool[pl.ds(EMPTY * 4, 4 * NB), :] = jnp.zeros((4 * NB, W), jnp.float32)
    mfpool[pl.ds(EMPTY, NB), :] = jnp.zeros((NB, W), jnp.float32)
    res[pl.ds(4 * NB, NB), :] = jnp.zeros((NB, W), jnp.float32)

    targets = [tgt[b] for b in range(NB)]
    ranks = []
    for b in range(NB):
        r = jnp.int32(0)
        for e in range(b):
            r = r + jnp.where(targets[e] == targets[b], 1, 0)
        ranks.append(r)
    places = [targets[b] * CAP + ranks[b] for b in range(NB)]
    for s in range(NG * CAP):
        found = jnp.int32(NB)
        for b in range(NB):
            found = jnp.where(places[b] == s, b, found)
        table[NG + g, s] = found

    @pl.when(jnp.logical_not(low))
    def _():
        for d in range(NG):
            for s in range(NG * CAP):
                table[d, s] = jnp.int32(NB)

    @pl.when(jnp.logical_not(high))
    def _():
        for d in range(NG):
            for s in range(NG * CAP):
                table[2 * NG + d, s] = jnp.int32(NB)

    def piece_at(ref, per, i, d):
        return ref.at[pl.ds(pl.multiple_of((i * NG + lax.rem(g + d, NG)) * per, per), per)]

    def over_group(ref, per, send, recv, d):
        part = piece_at(ref, per, 1, 0)
        return remote(part, part, load.at[send[0]], recv.at[NG - d - 1], at(a, lax.rem(g + d, NG)))

    def to_side(ref, per, send, recv, d, up):
        src, dst = piece_at(ref, per, 1, d), piece_at(ref, per, 0 if up else 2, d)
        k = 1 if up else 2
        return remote(src, dst, load.at[send[k]], recv.at[k + 2], at(a + (1 if up else -1), g))

    def sides(parts, d, do):
        for up, there in ((True, high), (False, low)):
            @pl.when(there)
            def _():
                for part in parts:
                    do(to_side(*part, d, up))

    def gathered(parts, between):
        for d in (2, 1, 3):
            for part in parts:
                over_group(*part, d).start()
        sides(parts, 0, lambda copy: copy.start())
        between()
        for d in (1, 3, 2):
            for ref, per, send, recv in parts:
                landed(ref.at[pl.ds(0, per)], recv.at[d - 1])
            sides(parts, d, lambda copy: copy.start())
        for k, there in ((3, low), (4, high)):
            @pl.when(there)
            def _():
                for ref, per, send, recv in parts:
                    landed(ref.at[pl.ds(0, NG * per)], recv.at[k])

    def sent(parts):
        for k, pieces, there in ((0, 3, None), (1, NG, high), (2, NG, low)):
            def left():
                for ref, per, send, recv in parts:
                    landed(ref.at[pl.ds(0, pieces * per)], load.at[send[k]])

            left() if there is None else pl.when(there)(left)

    first = ((pool, 4 * NB, (3, 4, 5), drecv), (table, 1, (6, 7, 2), trecv))

    def columns():
        rows[3 * NB : 4 * NB, :] = h * h

        def one(b, _):
            for comp in range(4):
                row = rows[pl.ds(comp * NB + b, 1), :]
                cols[comp, pl.ds(pl.multiple_of(b * W, W), W), :] = jnp.transpose(jnp.broadcast_to(row, (W, W)))
            return 0

        lax.fori_loop(0, NB, one, 0)

    gathered(first, columns)

    def partner(b, k):
        if k == 0:
            return NG + g, b
        n = nbr[k - 1, b]
        cell, s = n // 16, n % 16
        i, j = cell // 3, cell % 3
        t = tgt[b] + j - 1
        d = i * NG + s // CAP
        e = table[d, jnp.clip(t, 0, NG - 1) * CAP + s % CAP]
        there = (t >= 0) & (t < NG) & (a + i >= 1) & (a + i <= n_dom) & (e < NB)
        return jnp.where(there, d, 3 * NG), jnp.where(there, e, 0)

    def find(b):
        who = [partner(b, k) for k in range(5)]
        for k, (d, e) in enumerate(who):
            base_of[b * 5 + k] = d * NB + e
        return who

    lane_of = lax.broadcasted_iota(jnp.int32, (CH, W), 1)

    def keep(q, b, sums):
        here = slice(q * CH, (q + 1) * CH)
        kept = coll[here, :]
        for k, s in enumerate(sums):
            kept = jnp.where(lane_of == k * NB + b, jnp.sum(s, axis=1, keepdims=True), kept)
        coll[here, :] = kept

    def stashed(b, k, q):
        return pl.ds(pl.multiple_of((b * 5 + k) * W + q * CH, CH), CH)

    def density_pairs(b, _):
        who = find(b)
        for q in range(W // CH):
            mine_at = pl.ds(pl.multiple_of(b * W + q * CH, CH), CH)
            cx, cy, cz, ch2 = (cols[comp, mine_at, :] for comp in range(4))
            sums = [jnp.zeros((CH, W), jnp.float32) for _ in range(4)]
            for k, (d, e) in enumerate(who):
                base = d * (4 * NB) + e
                dx = cx - pool[pl.ds(base, 1), :]
                dy = cy - pool[pl.ds(base + NB, 1), :]
                dz = cz - pool[pl.ds(base + 2 * NB, 1), :]
                w = jnp.maximum(ch2 - (dx * dx + dy * dy + dz * dz), 0.0)
                w2 = w * w
                m_j = pool[pl.ds(base + 3 * NB, 1), :]
                parts = []
                for comp, delta in enumerate((dx, dy, dz)):
                    part = w2 * delta
                    stash[comp, stashed(b, k, q), :] = part
                    parts.append(m_j * part)
                parts.append(m_j * (w2 * w))
                sums = [s + p for s, p in zip(sums, parts)]
            keep(q, b, sums)
        return 0

    def force_pairs(b, _):
        who = [base_of[b * 5 + k] for k in range(5)]
        for q in range(W // CH):
            sums = [jnp.zeros((CH, W), jnp.float32) for _ in range(3)]
            for k, base in enumerate(who):
                mf_j = mfpool[pl.ds(base, 1), :]
                sums = [s + mf_j * stash[comp, stashed(b, k, q), :] for comp, s in enumerate(sums)]
            keep(q, b, sums)
        return 0

    def pairs(block):
        coll[...] = jnp.zeros((W, W), jnp.float32)
        def two(b, _):
            for k in range(4):
                block(4 * b + k, 0)
            return 0

        lax.fori_loop(0, NB // 4, two, 0)
        return jnp.transpose(coll[...])

    inv_h = 1.0 / h
    ih3 = inv_h * inv_h * inv_h
    ih9 = KNORM * (ih3 * ih3 * ih3)

    found = pairs(density_pairs)
    rho = ih9 * found[3 * NB : 4 * NB, :]
    factor = (GAMMA - 1.0) * u / rho
    mfpool[pl.ds(pl.multiple_of((NG + g) * NB, NB), NB), :] = m * factor
    res[0:NB, :] = rho
    for comp in range(3):
        res[(1 + comp) * NB : (2 + comp) * NB, :] = factor * found[comp * NB : (comp + 1) * NB, :]

    part = mfpool.at[pl.ds(pl.multiple_of((NG + g) * NB, NB), NB)]

    def factors(i):
        dst = mfpool.at[pl.ds(pl.multiple_of(((1 - i) * NG + g) * NB, NB), NB)]
        to = others if i == 0 else others + [g]
        return [
            remote(part, dst, load.at[i + 4], frecv.at[1 - i], at(a + i, o)) for k, o in enumerate(to)
        ]

    def on_sides(do):
        for i, there in ((1, high), (-1, low)):
            pl.when(there)(functools.partial(do, i))

    def start_factors(i):
        for copy in factors(i):
            copy.start()

    def sent_factors(i):
        landed(mfpool.at[pl.ds(0, (3 if i == 0 else NG) * NB)], load.at[i + 4])

    sent(first)
    on_sides(start_factors)
    start_factors(0)
    landed(mfpool.at[pl.ds(0, 3 * NB)], frecv.at[1])
    on_sides(lambda i: landed(mfpool.at[pl.ds(0, NG * NB)], frecv.at[1 + i]))

    found = pairs(force_pairs)
    for comp in range(3):
        here = slice((1 + comp) * NB, (2 + comp) * NB)
        total = 6.0 * ih9 * (res[here, :] + found[comp * NB : (comp + 1) * NB, :])
        res[here, :] = jnp.where(active, total, 0.0)

    @pl.when(root)
    def _():
        zbuf[pl.ds(z, 1), :] = mine[...]

        @pl.when(stand_in)
        def _():
            landed(zbuf.at[pl.ds(0, 2 * NZ - 1)], mrecv.at[0])

        @pl.when(jnp.logical_not(stand_in))
        def _():
            landed(zbuf.at[pl.ds(0, NZ - 1)], mrecv.at[0])

        least = jnp.min(zbuf[...], axis=0, keepdims=True)
        index = (y * 2 + c) * NG + g
        last[...] = least
        xbuf[pl.ds(index, 1), :] = least
        with_plane(lambda k, p: remote(last, xbuf.at[pl.ds(index, 1)], load.at[7], mrecv.at[1], p).start())

    for t in range(NG):
        for r in range(CAP):
            e = table[NG + g, t * CAP + r]
            for comp in range(4):
                source = jnp.where(e < NB, comp * NB + e, 4 * NB)
                outsend[t, comp * CAP + r : comp * CAP + r + 1, :] = res[pl.ds(source, 1), :]
    results = [remote(outsend.at[o], outbuf.at[g], load.at[6], orecv, at(a, o)) for o in others]
    for copy in results:
        copy.start()
    outbuf[g] = outsend[g]

    landed(outbuf.at[pl.ds(0, 3)], orecv)
    slots_out[...] = outbuf[...]

    sent_factors(0)
    on_sides(sent_factors)
    landed(outbuf.at[pl.ds(0, 3)], load.at[6])
    for zr, there in reports:
        pl.when(there)(lambda zr=zr: report(zr).wait_send())

    @pl.when(root)
    def _():
        @pl.when(z == 0)
        def _():
            landed(xbuf.at[pl.ds(0, len(moves) - 1)], load.at[7])

        @pl.when(z != 0)
        def _():
            landed(xbuf.at[pl.ds(0, len(moves))], load.at[7])

    @pl.when(root)
    def _():
        @pl.when(z == 0)
        def _():
            landed(xbuf.at[pl.ds(0, len(moves) - 1)], mrecv.at[1])

        @pl.when(z != 0)
        def _():
            landed(xbuf.at[pl.ds(0, len(moves))], mrecv.at[1])

        final[...] = jnp.min(xbuf[...], axis=0, keepdims=True)

    def give(k, to):
        return remote(final, final, load.at[k], mrecv.at[2], at(dom_of(to, y, c), g))

    @pl.when(z == 1)
    def _():
        for to in (4, 3, 2):
            give(2, to).start()
        pl.when(column)(lambda: give(7, 0).start())

    @pl.when(jnp.logical_not(root))
    def _():
        landed(final, mrecv.at[2])

    @pl.when(hands_on)
    def _():
        for to in range(NZ - 1, 4, -1):
            give(2, to).start()

    least_out[...] = final[...]

    @pl.when(z == 1)
    def _():
        landed(xbuf.at[pl.ds(0, 3)], load.at[2])
        pl.when(column)(lambda: landed(final, load.at[7]))

    @pl.when(hands_on)
    def _():
        landed(xbuf.at[pl.ds(0, NZ - 5)], load.at[2])


def unpack(slots_in, least_in, dens_out, acc_out, ts_out):
    for s in range(NG):
        dens_out[s * CAP : (s + 1) * CAP, :] = slots_in[s, 0:CAP, :]
        for comp in range(3):
            for r in range(CAP):
                row = (1 + comp) * CAP + r
                slot = s * CAP + r
                acc_out[comp : comp + 1, slot * W : (slot + 1) * W] = slots_in[s, row : row + 1, :]
    ts_out[0] = jnp.min(least_in[...])


def body(positions, velocity, smoothing, mass, energy, targets, neighbours, counts):
    f32 = jnp.float32
    slots = NG * CAP
    vmem, smem = pl.BlockSpec(memory_space=pltpu.VMEM), pl.BlockSpec(memory_space=pltpu.SMEM)
    sem = pltpu.SemaphoreType.DMA
    packed, least = pl.pallas_call(
        kernel,
        out_shape=(pltpu.VMEM((NG, 4 * CAP, W), f32), pltpu.VMEM((1, W), f32)),
        in_specs=[pl.BlockSpec(memory_space=pl.ANY)] * 8,
        out_specs=(vmem, vmem),
        scratch_shapes=[
            pltpu.SMEM((NB,), jnp.int32),
            pltpu.SMEM((4, NB), jnp.int32),
            pltpu.SMEM((NB,), jnp.int32),
            pltpu.VMEM((3, NB * W), f32),
            pltpu.VMEM((3, NB * W), f32),
            pltpu.VMEM((NB, W), f32),
            pltpu.VMEM((NB, W), f32),
            pltpu.VMEM((NB, W), f32),
            pltpu.SMEM((5 * NB,), jnp.int32),
            pltpu.VMEM(((EMPTY + NB) * 4, W), f32),
            pltpu.VMEM((EMPTY + NB, W), f32),
            pltpu.SMEM((3 * NG, 16), jnp.int32),
            pltpu.VMEM((4 * NB, W), f32),
            pltpu.VMEM((4, NB * W, W), f32),
            pltpu.VMEM((3, 5 * NB * W, W), f32),
            pltpu.VMEM((W, W), f32),
            pltpu.VMEM((5 * NB, W), f32),
            pltpu.VMEM((NG, 4 * CAP, W), f32),
            pltpu.VMEM((NG, 4 * CAP, W), f32),
            pltpu.VMEM((1, W), f32),
            pltpu.VMEM((2 * NZ, W), f32),
            pltpu.VMEM((2 * NY * NG, W), f32),
            pltpu.VMEM((1, W), f32),
            pltpu.VMEM((1, W), f32),
            sem((8,)), sem((5,)), sem((5,)), sem((3,)), sem, sem((3,)),
        ],
        compiler_params=pltpu.CompilerParams(collective_id=0, has_side_effects=True),
    )(
        targets.reshape(-1), neighbours.T, counts, positions, velocity,
        smoothing.reshape(NB, W), mass.reshape(NB, W), energy.reshape(NB, W),
    )
    dens, acc, ts = pl.pallas_call(
        unpack,
        out_shape=(
            jax.ShapeDtypeStruct((slots, W), f32),
            jax.ShapeDtypeStruct((3, slots * W), f32),
            jax.ShapeDtypeStruct((1,), f32),
        ),
        in_specs=[vmem] * 2,
        out_specs=(vmem, vmem, smem),
    )(*(pltpu.with_memory_space_constraint(v, pltpu.VMEM) for v in (packed, least)))
    return dens.reshape(-1), acc, ts


def solution(mesh):
    both = ("dom", "grp")
    return jax.shard_map(
        body,
        mesh=mesh,
        in_specs=(P(None, both), P(None, both), P(both), P(both), P(both), P(both, None), P(both, None), P(both)),
        out_specs=(P(both), P(None, both), P()),
        check_vma=False,
    )
```
